256 devices in a mesh: patch: 8 (over x, core), space: 32 (over z, y).
Axes of the slice: x: 4, y: 4, z: 8, core: 2. Of those that a mesh axis runs over, the one named last changes fastest.
Arguments:
- image: bfloat16 [64, 64, 256], P('patch', 'space'), may hold values from -6 to 6
- offsets: int32 [8, 2], replicated, may hold values from 0 to 128, as said below
- conv1_weight: bfloat16 [9, 32, 3], replicated, may hold values from -1.25 to 1.25
- conv2_weight: bfloat16 [9, 32, 96], replicated, may hold values from -0.21875 to 0.21875
- norm1_gain: float32 [32], replicated, may hold values from 0.1 to 1.9
- norm1_bias: float32 [32], replicated, may hold values from -3 to 3
- norm2_gain: float32 [32], replicated, may hold values from 0.1 to 1.9
- norm2_bias: float32 [32], replicated, may hold values from -3 to 3
- head_weight: bfloat16 [3, 32], replicated, may hold values from -1 to 1
- head_bias: float32 [3], replicated, may hold values from -3 to 3
Outputs:
- volume_logits: float32 [64, 3, 64, 256], P('patch', None, 'space')
The draws below stay inside these ranges and needn't reach their ends.
Inputs may be any that keep to these rules, and one draw needn't show every extreme that they name: offsets[p] = (oz, ox) with 0 <= oz <= 48 and 0 <= ox <= 128; some patch starts at oz = 48, some at ox = 128, some at ox = 0.
All inputs are finite; a program needn't handle non-finite values.
Results may differ from the reference program's by a relative error of at most 0.0024.
Values may be sent and summed in bfloat16 or wider, within the bound.
A program may use at most 64 MiB of HBM per device.

```python
import jax
import jax.numpy as jnp
from jax import lax

CH = 32
CLASSES = 3
PX = 128
PZ = 16
PATCHES = 8
PY = 64
VZ = 64
VX = 256


def draw_offsets(key, part):
    depth_room = VZ - PZ
    width_room = VX - PX
    draw_one = jax.random.randint(jax.random.fold_in(key, 11), (PATCHES,), 0, depth_room + 1)
    draw_two = jax.random.randint(jax.random.fold_in(key, 12), (PATCHES,), 0, depth_room + 1)
    depths = (draw_one + draw_two) // 2
    across = jax.random.randint(jax.random.fold_in(key, 13), (PATCHES,), 0, width_room + 1)
    deep_index = jax.random.randint(jax.random.fold_in(key, 14), (), 0, PATCHES)
    wide_index = jax.random.randint(jax.random.fold_in(key, 15), (), 0, PATCHES)
    step_index = jax.random.randint(jax.random.fold_in(key, 16), (), 0, PATCHES - 1)
    left_index = (wide_index + 1 + step_index) % PATCHES
    depths = depths.at[deep_index].set(depth_room)
    across = across.at[wide_index].set(width_room)
    across = across.at[left_index].set(0)
    return jnp.stack([depths, across], axis=1).astype(jnp.int32)


def shard_levels(key, shape, pieces, smallest, top_value):
    def one(dim, parts):
        heights = jax.random.uniform(jax.random.fold_in(jax.random.fold_in(key, 6), dim), (parts,), jnp.float32, smallest / len(pieces), top_value / len(pieces))
        return jnp.repeat(jnp.exp(heights), shape[dim] // parts).reshape((-1,) + (1,) * (len(shape) - dim - 1))

    loudness = one(*pieces[0])
    for cut in pieces[1:]:
        loudness = loudness * one(*cut)
    return loudness


def centred(rng, dims, scale, bound, pieces=(), kind=jnp.bfloat16):
    array = jax.random.normal(rng, dims, jnp.float32) * scale
    if len(pieces) > 0:
        array = shard_levels(rng, dims, pieces, -0.22, 0.18) * array
    return jnp.clip(array, min=-bound, max=bound).astype(kind)


def setup_inputs(seed: int = 0) -> dict:
    key_of = jax.random.split(jax.random.key(seed), 11)
    return {
        "image": centred(key_of[0], (VZ, PY, VX), 1.0, 6.0, ((0, 8), (1, 32))),
        "offsets": draw_offsets(jax.random.fold_in(key_of[10], 71), 0),
        "conv1_weight": centred(key_of[2], (9, CH, 3), 27 ** -0.5, 1.25),
        "conv2_weight": centred(key_of[3], (9, CH, 3 * CH), (27 * CH) ** -0.5, 0.21875),
        "norm1_gain": jnp.clip(1.0 + 0.18 * jax.random.normal(key_of[4], (CH,), jnp.float32), 0.1, 1.9),
        "norm1_bias": centred(key_of[5], (CH,), 0.5, 3.0, (), jnp.float32),
        "norm2_gain": jnp.clip(1.0 + 0.18 * jax.random.normal(key_of[6], (CH,), jnp.float32), 0.1, 1.9),
        "norm2_bias": centred(key_of[7], (CH,), 0.5, 3.0, (), jnp.float32),
        "head_weight": centred(key_of[8], (CLASSES, CH), CH ** -0.5, 1.0),
        "head_bias": centred(key_of[9], (CLASSES,), 0.5, 3.0, (), jnp.float32),
    }


def gauss_value(positions, length):
    center = (length - 1) / 2.0
    deviation = length / 8.0
    offset = positions - center
    return jnp.exp(-(offset * offset) / (2.0 * deviation * deviation))

def apply_taps(padded, weights):
    depth_cells = padded.shape[2] - 2
    row_cells = padded.shape[3] - 2
    col_cells = padded.shape[4] - 2
    stacked = jnp.concatenate([padded[:, :, :, :, col_shift:col_shift + col_cells] for col_shift in range(3)], axis=1)
    summed = jnp.zeros((padded.shape[0], weights.shape[1], depth_cells, row_cells, col_cells), jnp.float32)
    for depth_tap in range(3):
        for row_tap in range(3):
            window = stacked[:, :, depth_tap:depth_tap + depth_cells, row_tap:row_tap + row_cells, :]
            summed = summed + jnp.einsum('oc,fczyx->fozyx', weights[depth_tap * 3 + row_tap].astype(jnp.float32), window.astype(jnp.float32))
    return summed

def convolve(features, weights):
    padded = jnp.pad(features, ((0, 0), (0, 0), (1, 1), (1, 1), (1, 1)))
    return apply_taps(padded, weights)

def normalize(values, channel_gain, channel_bias):
    average = lax.optimization_barrier(jnp.mean(values, axis=(2, 3, 4)))
    centered = values - average[:, :, None, None, None]
    variance = lax.optimization_barrier(jnp.mean(centered * centered, axis=(2, 3, 4)))
    factor = lax.rsqrt(variance + 1e-05) * channel_gain[None, :]
    shifted = centered * factor[:, :, None, None, None] + channel_bias[None, :, None, None, None]
    return jnp.where(shifted >= 0, shifted, 0.01 * shifted).astype(jnp.bfloat16)

def run_network(patch_cells, conv1_weight, conv2_weight, norm1_gain, norm1_bias, norm2_gain, norm2_bias, head_weight, head_bias):
    flipped = jnp.stack([patch_cells, patch_cells[::-1], patch_cells[:, :, ::-1], patch_cells[::-1, :, ::-1]])[:, None]
    hidden = normalize(convolve(flipped, conv1_weight), norm1_gain, norm1_bias)
    hidden = normalize(convolve(hidden, conv2_weight), norm2_gain, norm2_bias)
    logits = jnp.einsum('kc,fczyx->fzkyx', head_weight.astype(jnp.float32), hidden.astype(jnp.float32))
    logits = logits + head_bias[None, None, :, None, None]
    restored = logits[0] + logits[1][::-1] + logits[2][:, :, :, ::-1] + logits[3][::-1, :, :, ::-1]
    return restored * 0.25

def reference(image, offsets, conv1_weight, conv2_weight, norm1_gain, norm1_bias, norm2_gain, norm2_bias, head_weight, head_bias):
    gauss_depth = gauss_value(jnp.arange(PZ, dtype=jnp.float32), PZ)
    gauss_rows = gauss_value(jnp.arange(PY, dtype=jnp.float32), PY)
    gauss_cols = gauss_value(jnp.arange(PX, dtype=jnp.float32), PX)
    weight_map = gauss_depth[:, None, None] * gauss_rows[None, :, None] * gauss_cols[None, None, :]

    def one_patch(item_index, carried):
        blended, coverage = carried
        corner = lax.dynamic_index_in_dim(offsets, item_index, 0, keepdims=False).astype(jnp.int32)
        start_z = corner[0]
        start_x = corner[1]
        zero_index = jnp.zeros((), jnp.int32)
        patch_cells = lax.dynamic_slice(image, (start_z, zero_index, start_x), (PZ, PY, PX))
        averaged = run_network(patch_cells, conv1_weight, conv2_weight, norm1_gain, norm1_bias, norm2_gain, norm2_bias, head_weight, head_bias)
        contrib = averaged * weight_map[:, None, :, :]
        current = lax.dynamic_slice(blended, (start_z, zero_index, zero_index, start_x), contrib.shape)
        blended = lax.dynamic_update_slice(blended, current + contrib, (start_z, zero_index, zero_index, start_x))
        present = lax.dynamic_slice(coverage, (start_z, zero_index, start_x), weight_map.shape)
        coverage = lax.dynamic_update_slice(coverage, present + weight_map, (start_z, zero_index, start_x))
        return (blended, coverage)
    start_blend = jnp.zeros((VZ, CLASSES, PY, VX), jnp.float32)
    start_cover = jnp.zeros((VZ, PY, VX), jnp.float32)
    blended, coverage = lax.fori_loop(0, PATCHES, one_patch, (start_blend, start_cover))
    return blended / jnp.maximum(coverage, 0.1)[:, None, :, :]
```

```python
import jax
import jax.numpy as jnp
from jax import lax
from jax.experimental import pallas as pl
from jax.experimental.pallas import tpu as pltpu
from jax.sharding import PartitionSpec as P

PX = 128
PZ = 16
CH = 32
NP = 8
NS = 32
PY = 64
VX = 256
MESH = pl.DeviceIdType.MESH
BF = jnp.bfloat16
F32 = jnp.float32
HI = lax.Precision.HIGHEST


def iota(shape, dim):
    return lax.broadcasted_iota(jnp.int32, shape, dim)


def gauss(positions, length):
    center = (length - 1) / 2.0
    deviation = length / 8.0
    offset = positions - center
    return jnp.exp(-(offset * offset) / (2.0 * deviation * deviation))


def kernel(
    image, offs, w1, w2, g1, b1, g2, b2, hw, hb, out,
    slab, xsend, gath, w1s, w2s, whs, sels, im2, own, halo, act, pbuf, conv, hid,
    st1, st2, unblend, place, inv, wmap, logit, msend, mrecv,
    s_img, r_img, s_st1, r_st1, s_st2, r_st2, s_out, r_out,
):
    me = lax.axis_index("patch")
    sp = lax.axis_index("space")

    def space(k):
        return lax.rem(sp + k + NS, NS)

    def group(k):
        return lax.rem(me + k, NP)

    barrier = pltpu.get_barrier_semaphore()

    def greet(p, s):
        pl.semaphore_signal(barrier, inc=1, device_id=(p, s), device_id_type=MESH)

    def greet_space(k, c):
        greet(me, space(k))
        return c

    lax.fori_loop(1, NS, greet_space, 0)

    def greet_group(k, c):
        greet(group(k), sp)
        greet(group(k), space(1))
        greet(group(k), space(-1))
        return c

    lax.fori_loop(1, NP, greet_group, 0)

    for z in range(8):
        slab[2 * z : 2 * z + 2, :] = image[z].astype(F32)
    diff = iota((VX, PX), 0) - iota((VX, PX), 1)
    for p in range(NP):
        pick = jnp.where(diff == offs[p, 1], 1.0, 0.0).astype(BF)
        xsend[p] = jnp.dot(slab[...].astype(BF), pick, preferred_element_type=F32).astype(BF)

    pl.semaphore_wait(barrier, NS - 1 + 3 * (NP - 1))

    def image_copy(n, p):
        return pltpu.make_async_remote_copy(
            src_ref=xsend.at[p], dst_ref=gath.at[n, me],
            send_sem=s_img.at[n, p], recv_sem=r_img.at[n, me],
            device_id=(p, space(1 - n)), device_id_type=MESH,
        )

    def image_arrival(n, q):
        return pltpu.make_async_remote_copy(
            src_ref=xsend.at[q], dst_ref=gath.at[n, q],
            send_sem=s_img.at[n, q], recv_sem=r_img.at[n, q],
            device_id=(q, space(1 - n)), device_id_type=MESH,
        )

    def send_images(k, c):
        image_copy(0, group(k)).start()
        image_copy(2, group(k)).start()
        image_copy(1, group(k)).start()
        return c

    lax.fori_loop(1, NP, send_images, 0)
    image_copy(0, me).start()
    image_copy(2, me).start()
    gath[1, me] = xsend[me]

    lane = iota((CH, VX), 1)
    for flip in range(2):
        base = jnp.zeros((CH, VX), F32)
        for a in range(3):
            for b in range(3):
                taps = w1[3 * a + b].astype(F32)
                for c in range(3):
                    where = c * 48 + b * 8 + (2 - a if flip else a)
                    base = base + jnp.where(lane == where, taps[:, c : c + 1], 0.0)
        for part in range(2):
            for zo in range(4):
                for r in range(2):
                    row = (1 + r) if part == 0 else 3 * r
                    shift = row * 8 + zo
                    moved = base if shift == 0 else pltpu.roll(base, shift, 1)
                    at = part * 512 + flip * 256 + zo * 64 + r * 32
                    w1s[at : at + 32, :] = moved[:, :144].astype(BF)
    nothing = jnp.zeros((CH, 96), F32)
    for a in range(3):
        taps = [w2[3 * a + b].astype(F32) for b in range(3)]
        for ro in range(2):
            pieces = [nothing] + taps if ro else taps + [nothing]
            block = jnp.concatenate(pieces, axis=1).astype(BF)
            for zp in range(2):
                slot = zp - a + 2
                if 0 <= slot < 4:
                    at = (slot * 2 + ro) * 32
                    w2s[at : at + 32, zp * 384 : zp * 384 + 384] = block
    for slot, zp in ((3, 0), (0, 1)):
        w2s[slot * 64 : slot * 64 + 64, zp * 384 : zp * 384 + 384] = jnp.zeros((64, 384), BF)

    oz = offs[me, 0]
    rows = iota((48, 384), 0)
    cols = iota((48, 384), 1)
    slot_n = lax.shift_right_logical(cols, 7)
    from_z = lax.shift_right_logical(cols & 127, 1)
    from_row = slot_n * 2 + (cols & 1)
    to_row = lax.shift_right_logical(rows, 3)
    low = jnp.where(sp == 0, 2, 0)
    high = jnp.where(sp == NS - 1, 3, 5)
    keep_row = (from_row == to_row) & (to_row >= low) & (to_row <= high)
    for b in range(4):
        rel = (rows & 7) + (4 * b - 1)
        hit = keep_row & (from_z == rel + oz) & (rel >= 0) & (rel < PZ)
        sels[b * 48 : b * 48 + 48, :] = jnp.where(hit, 1.0, 0.0).astype(BF)

    for n in range(3):
        def wait_image(q, c, n=n):
            image_arrival(n, q).wait_recv()
            return c
        if n == 1:
            lax.fori_loop(1, NP, lambda k, c: wait_image(group(k), c), 0)
        else:
            lax.fori_loop(0, NP, wait_image, 0)

    rowsel = jnp.dot(sels[...], gath[...].reshape(384, PX), preferred_element_type=F32)
    lane_r = iota((192, PX), 1)
    before = jnp.where(lane_r == 0, 0.0, pltpu.roll(rowsel, 1, 1))
    after = jnp.where(lane_r == PX - 1, 0.0, pltpu.roll(rowsel, PX - 1, 1))
    for c, cells in enumerate((before, rowsel, after)):
        for b in range(4):
            cut = cells[b * 48 : b * 48 + 48].astype(BF)
            im2[c * 48 : c * 48 + 48, b * PX : b * PX + PX] = cut
            im2[(2 - c) * 48 : (2 - c) * 48 + 48, 512 + b * PX : 512 + b * PX + PX] = cut

    def sums(parts):
        first = parts[0]
        second = parts[0] * parts[0]
        for part in parts[1:]:
            first = first + part
            second = second + part * part
        return first, second

    def to_lanes(blocks):
        cells = jnp.concatenate(blocks, axis=0)
        return jnp.sum(jnp.transpose(cells), axis=0, keepdims=True)

    own[...] = jnp.dot(w1s[:512], im2[...], preferred_element_type=F32)
    firsts, seconds = [], []
    for zf in range(2):
        for xf in range(2):
            one, two = sums([
                own[zf * 256 + i * 32 : zf * 256 + i * 32 + 32, xf * 512 + b * PX : xf * 512 + b * PX + PX]
                for i in range(8) for b in range(4)
            ])
            firsts.append(one)
            seconds.append(two)

    def stat_copy(buf, ssem, rsem, k):
        return pltpu.make_async_remote_copy(
            src_ref=buf.at[sp], dst_ref=buf.at[sp],
            send_sem=ssem.at[k], recv_sem=rsem.at[sp],
            device_id=(me, space(k)), device_id_type=MESH,
        )

    def stat_arrival(buf, ssem, rsem, k):
        return pltpu.make_async_remote_copy(
            src_ref=buf.at[space(k)], dst_ref=buf.at[space(k)],
            send_sem=ssem.at[k], recv_sem=rsem.at[space(k)],
            device_id=(me, space(k)), device_id_type=MESH,
        )

    def send_stats(buf, ssem, rsem):
        def body(k, c):
            stat_copy(buf, ssem, rsem, lax.rem(k + 15, NS - 1) + 1).start()
            return c
        lax.fori_loop(0, NS - 1, body, 0)

    def wait_stats(buf, ssem, rsem):
        def body(k, c):
            stat_arrival(buf, ssem, rsem, k).wait_recv()
            return c
        lax.fori_loop(1, NS, body, 0)

    def scales(buf, gain, bias):
        total = jnp.sum(buf[...], axis=0)
        cells = float(PZ * PY * PX)
        mean = total[0:1] / cells
        variance = total[1:2] / cells - mean * mean
        factor = lax.rsqrt(variance + 1e-05) * jnp.concatenate([gain[...]] * 4, axis=1)
        shift = jnp.concatenate([bias[...]] * 4, axis=1) - mean * factor
        return (
            jnp.transpose(jnp.broadcast_to(factor, (128, 128))),
            jnp.transpose(jnp.broadcast_to(shift, (128, 128))),
        )

    def leaky(u):
        return jnp.maximum(u, 0.01 * u)

    st1[sp] = jnp.concatenate([to_lanes(firsts), to_lanes(seconds)], axis=0)
    send_stats(st1, s_st1, r_st1)

    halo[...] = jnp.dot(w1s[512:], im2[...], preferred_element_type=F32)

    row16 = iota((16, 512), 0)
    col16 = iota((16, 512), 1)
    head = jnp.concatenate([hw[...].astype(F32)] * 16, axis=1)
    k16 = lax.shift_right_logical(row16 & 7, 1)
    spread = jnp.zeros((16, 512), F32)
    for k in range(3):
        spread = jnp.where(k16 == k, head[k : k + 1, :], spread)
    same = (lax.shift_right_logical(row16, 3) == (lax.shift_right_logical(col16, 6) & 1)) & (
        (row16 & 1) == (lax.shift_right_logical(col16, 5) & 1)
    )
    whs[...] = jnp.where(same, spread, 0.0).astype(BF)

    lead = iota((128, PX), 0)
    width = iota((128, PX), 1)
    row_y = (2 * sp + (lead & 1)).astype(F32)
    wmap[...] = (
        gauss(lax.shift_right_logical(lead, 3).astype(F32), PZ) * gauss(row_y, PY) * gauss(width.astype(F32), PX)
    )

    r48 = iota((48, 128), 0)
    c48 = iota((48, 128), 1)
    z48 = lax.shift_right_logical(r48 * 43, 8)
    m48 = r48 - z48 * 6
    for q in range(NP):
        hit = ((c48 & 7) == m48) & (lax.shift_right_logical(c48, 3) == z48 + 8 * q - oz)
        place[q * 48 : q * 48 + 48, :] = jnp.where(hit, 1.0, 0.0).astype(BF)

    rc = iota((48, VX), 0)
    xc = iota((48, VX), 1)
    zc = lax.shift_right_logical(rc * 43, 8)
    yc = (2 * sp + ((rc - zc * 6) & 1)).astype(F32)
    plane = jnp.zeros((48, VX), F32)
    for p in range(NP):
        rel_z = 8 * me + zc - offs[p, 0]
        rel_x = xc - offs[p, 1]
        inside = (rel_z >= 0) & (rel_z < PZ) & (rel_x >= 0) & (rel_x < PX)
        value = gauss(rel_z.astype(F32), PZ) * gauss(rel_x.astype(F32), PX)
        plane = plane + jnp.where(inside, value, 0.0)
    inv[...] = jnp.maximum(plane * gauss(yc, PY), 0.1)

    back = iota((PX, VX), 1) - iota((PX, VX), 0)
    for p in range(NP):
        unblend[p * PX : p * PX + PX, :] = jnp.where(back == offs[p, 1], 1.0, 0.0).astype(BF)

    wait_stats(st1, s_st1, r_st1)
    factor1, shift1 = scales(st1, g1, b1)

    edge = (jnp.where(sp == 0, 0.0, 1.0), jnp.where(sp == NS - 1, 0.0, 1.0))
    lane_b = iota((CH, PX), 1)
    firsts, seconds = [], []
    for zf in range(2):
        for xf in range(2):
            f = zf * 2 + xf
            scale = factor1[f * 32 : f * 32 + 32]
            shift = shift1[f * 32 : f * 32 + 32]
            for zo in range(4):
                for row in range(4):
                    source = own if row in (1, 2) else halo
                    r = row - 1 if row in (1, 2) else row // 3
                    at = zf * 256 + zo * 64 + r * 32
                    if row in (0, 3):
                        sc, sh = scale * edge[row // 3], shift * edge[row // 3]
                    else:
                        sc, sh = scale, shift
                    zp = zo % 2
                    zi = 1 - zp if zf else zp
                    for b in range(4):
                        j = 2 * b + zo // 2
                        u = leaky(source[at : at + 32, xf * 512 + b * PX : xf * 512 + b * PX + PX] * sc + sh)
                        prior = jnp.where(lane_b == 0, 0.0, pltpu.roll(u, 1, 1))
                        later = jnp.where(lane_b == PX - 1, 0.0, pltpu.roll(u, PX - 1, 1))
                        for c, cells in enumerate((prior, u, later)):
                            ci = 2 - c if xf else c
                            k = ((zi * 4 + row) * 3 + ci) * 32
                            act[k : k + 32, f * 1024 + j * PX : f * 1024 + j * PX + PX] = cells.astype(BF)
            pbuf[...] = jnp.dot(w2s[...], act[:, f * 1024 : f * 1024 + 1024], preferred_element_type=F32)

            def slot(s, j):
                s = 3 - s if zf else s
                return pbuf[s * 64 : s * 64 + 64, j * PX : j * PX + PX]

            parts = []
            for j in range(8):
                even = slot(1, j)
                if j > 0:
                    even = even + slot(3, j - 1)
                odd = slot(2, j)
                if j < 7:
                    odd = odd + slot(0, j + 1)
                for zp, value in enumerate((even, odd)):
                    at = f * 128 + zp * 64
                    conv[at : at + 64, j * PX : j * PX + PX] = value
                    parts.append(value[:32])
                    parts.append(value[32:])
            one, two = sums(parts)
            firsts.append(one)
            seconds.append(two)

    st2[sp] = jnp.concatenate([to_lanes(firsts), to_lanes(seconds)], axis=0)
    send_stats(st2, s_st2, r_st2)
    wait_stats(st2, s_st2, r_st2)
    factor2, shift2 = scales(st2, g2, b2)

    for f in range(4):
        scale = factor2[f * 32 : f * 32 + 32]
        shift = shift2[f * 32 : f * 32 + 32]
        for i in range(4):
            at = f * 128 + i * 32
            for j in range(8):
                u = leaky(conv[at : at + 32, j * PX : j * PX + PX] * scale + shift)
                hid[at : at + 32, j * PX : j * PX + PX] = u.astype(BF)
    raw = jnp.dot(whs[...], hid[...], preferred_element_type=F32)
    k_of = lax.shift_right_logical(iota((16, PX), 0) & 7, 1)
    head_b = jnp.where(k_of == 0, hb[0], jnp.where(k_of == 1, hb[1], hb[2]))
    for j in range(8):
        value = (raw[:, j * PX : j * PX + PX] * 0.25 + head_b) * wmap[j * 16 : j * 16 + 16, :]
        logit[j * 16 : j * 16 + 16, :] = value.astype(BF)
    placed = jnp.dot(place[...], logit[...], preferred_element_type=F32)
    for q in range(NP):
        msend[q] = placed[q * 48 : q * 48 + 48].astype(BF)

    def out_copy(q):
        return pltpu.make_async_remote_copy(
            src_ref=msend.at[q], dst_ref=mrecv.at[me],
            send_sem=s_out.at[q], recv_sem=r_out.at[me],
            device_id=(q, sp), device_id_type=MESH,
        )

    def out_arrival(q):
        return pltpu.make_async_remote_copy(
            src_ref=msend.at[q], dst_ref=mrecv.at[q],
            send_sem=s_out.at[q], recv_sem=r_out.at[q],
            device_id=(q, sp), device_id_type=MESH,
        )

    def send_out(k, c):
        out_copy(group(k)).start()
        return c

    lax.fori_loop(1, NP, send_out, 0)
    mrecv[me] = msend[me]

    def wait_out(k, c):
        out_arrival(group(k)).wait_recv()
        return c

    lax.fori_loop(1, NP, wait_out, 0)
    got = jnp.concatenate([mrecv[p] for p in range(NP)], axis=1)
    final = jnp.dot(got, unblend[...], preferred_element_type=F32) / inv[...]
    for z in range(8):
        for k in range(3):
            out[z, k] = final[z * 6 + k * 2 : z * 6 + k * 2 + 2, :]

    def drain_images(k, c):
        image_copy(0, group(k)).wait_send()
        image_copy(2, group(k)).wait_send()
        image_copy(1, group(k)).wait_send()
        return c

    lax.fori_loop(1, NP, drain_images, 0)
    image_copy(0, me).wait_send()
    image_copy(2, me).wait_send()

    def drain_stats(k, c):
        stat_copy(st1, s_st1, r_st1, k).wait_send()
        stat_copy(st2, s_st2, r_st2, k).wait_send()
        return c

    lax.fori_loop(1, NS, drain_stats, 0)

    def drain_out(k, c):
        out_copy(group(k)).wait_send()
        return c

    lax.fori_loop(1, NP, drain_out, 0)


def local(image, offsets, w1, w2, g1, b1, g2, b2, hw, hb):
    vm = pl.BlockSpec(memory_space=pltpu.VMEM)
    sm = pl.BlockSpec(memory_space=pltpu.SMEM)
    dma = pltpu.SemaphoreType.DMA
    return pl.pallas_call(
        kernel,
        out_shape=jax.ShapeDtypeStruct((8, 3, 2, VX), F32),
        in_specs=[vm, sm, vm, vm, vm, vm, vm, vm, vm, sm],
        out_specs=vm,
        scratch_shapes=[
            pltpu.VMEM((16, VX), F32),
            pltpu.VMEM((NP, 16, PX), BF),
            pltpu.VMEM((3, NP, 16, PX), BF),
            pltpu.VMEM((1024, 144), BF),
            pltpu.VMEM((256, 768), BF),
            pltpu.VMEM((16, 512), BF),
            pltpu.VMEM((192, 384), BF),
            pltpu.VMEM((144, 1024), BF),
            pltpu.VMEM((512, 1024), F32),
            pltpu.VMEM((512, 1024), F32),
            pltpu.VMEM((768, 4096), BF),
            pltpu.VMEM((256, 1024), F32),
            pltpu.VMEM((512, 1024), F32),
            pltpu.VMEM((512, 1024), BF),
            pltpu.VMEM((NS, 2, PX), F32),
            pltpu.VMEM((NS, 2, PX), F32),
            pltpu.VMEM((1024, VX), BF),
            pltpu.VMEM((384, PX), BF),
            pltpu.VMEM((48, VX), F32),
            pltpu.VMEM((128, PX), F32),
            pltpu.VMEM((128, PX), BF),
            pltpu.VMEM((NP, 48, PX), BF),
            pltpu.VMEM((NP, 48, PX), BF),
            dma((3, NP)), dma((3, NP)),
            dma((NS,)), dma((NS,)), dma((NS,)), dma((NS,)),
            dma((NP,)), dma((NP,)),
        ],
        compiler_params=pltpu.CompilerParams(collective_id=0, has_side_effects=True, vmem_limit_bytes=60 * 1024 * 1024),
    )(
        image, offsets, w1, w2, g1.reshape(1, CH), b1.reshape(1, CH), g2.reshape(1, CH), b2.reshape(1, CH), hw, hb,
    )


def solution(mesh):
    return jax.shard_map(
        local,
        mesh=mesh,
        in_specs=(P("patch", "space", None), P(), P(), P(), P(), P(), P(), P(), P(), P()),
        out_specs=P("patch", None, "space", None),
        check_vma=False,
    )
```

```python
import jax
import jax.numpy as jnp
from jax import lax
from jax.experimental import pallas as pl
from jax.experimental.pallas import tpu as pltpu
from jax.sharding import PartitionSpec as P

PX = 128
PZ = 16
CH = 32
NP = 8
NS = 32
PY = 64
VX = 256
MESH = pl.DeviceIdType.MESH
BF = jnp.bfloat16
F32 = jnp.float32
HI = lax.Precision.HIGHEST


def iota(shape, dim):
    return lax.broadcasted_iota(jnp.int32, shape, dim)


def gauss(positions, length):
    center = (length - 1) / 2.0
    deviation = length / 8.0
    offset = positions - center
    return jnp.exp(-(offset * offset) / (2.0 * deviation * deviation))


def far(k):
    dz = (k + 1) // 4
    return -min(dz, 8 - dz) - min(k % 4, 4 - k % 4)


def kernel(
    image_in, offs_in, w1_in, w2_in, g1_in, b1_in, g2_in, b2_in, hw_in, hb_in, mrecv, unblend, inv,
    image, offs, w1, w2, g1, b1, g2, b2, hw, hb, wrow, slab, xsend, gath, w1s, w2s, whs, sels, im2, own, halo, act, pbuf, conv, hid,
    st1, st2, place, wmap, logit, msend,
    s_in, s_img, r_img, s_st1, r_st1, s_st2, r_st2, s_out, r_out,
):
    me = lax.axis_index("patch")
    sp = lax.axis_index("space")

    def space(k):
        return lax.rem(sp + k + NS, NS)

    def group(k):
        return lax.rem(me + k, NP)

    barrier = pltpu.get_barrier_semaphore()

    def greet(p, s):
        pl.semaphore_signal(barrier, inc=1, device_id=(p, s), device_id_type=MESH)

    for k in sorted(range(1, NS), key=far):
        greet(me, space(k))
    for k in (4, 5, 3, 2, 6, 7, 1):
        greet(group(k), space(1))
        greet(group(k), space(-1))
        greet(group(k), sp)

    pairs = (
        (image_in, image), (offs_in, offs), (w1_in, w1), (w2_in, w2), (g1_in, g1),
        (b1_in, b1), (g2_in, g2), (b2_in, b2), (hw_in, hw), (hb_in, hb),
    )
    loads = [pltpu.make_async_copy(src, dst, s_in.at[i]) for i, (src, dst) in enumerate(pairs)]
    for load in loads:
        load.start()
    wrow[...] = jnp.zeros_like(wrow)
    for load in loads[:2]:
        load.wait()

    for z in range(8):
        slab[2 * z : 2 * z + 2, :] = image[z].astype(F32)
    diff = iota((VX, PX), 0) - iota((VX, PX), 1)
    for p in range(NP):
        pick = jnp.where(diff == offs[1, p], 1.0, 0.0).astype(BF)
        xsend[p] = jnp.dot(slab[...].astype(BF), pick, preferred_element_type=F32).astype(BF)

    pl.semaphore_wait(barrier, NS - 1 + 3 * (NP - 1))

    def image_copy(n, p):
        return pltpu.make_async_remote_copy(
            src_ref=xsend.at[p], dst_ref=gath.at[n, me],
            send_sem=s_img.at[n, p], recv_sem=r_img.at[n, me],
            device_id=(p, space(1 - n)), device_id_type=MESH,
        )

    def image_arrival(n, q):
        return pltpu.make_async_remote_copy(
            src_ref=xsend.at[q], dst_ref=gath.at[n, q],
            send_sem=s_img.at[n, q], recv_sem=r_img.at[n, q],
            device_id=(q, space(1 - n)), device_id_type=MESH,
        )

    def send_images(k, c):
        image_copy(0, group(k)).start()
        image_copy(2, group(k)).start()
        image_copy(1, group(k)).start()
        return c

    lax.fori_loop(1, NP, send_images, 0)
    image_copy(0, me).start()
    image_copy(2, me).start()
    gath[1, me] = xsend[me]

    for load in loads[2:]:
        load.wait()
    for t in range(9):
        wrow[3 * t : 3 * t + 3, :] = w1[t].astype(F32)
    lane = iota((CH, VX), 1)
    tap = iota((CH, VX), 0)
    tap_a = lax.shift_right_logical(tap * 57, 9)
    tap_r = tap - 9 * tap_a
    tap_b = lax.shift_right_logical(tap_r * 11, 5)
    tap_c = tap_r - 3 * tap_b
    for flip in range(2):
        where = tap_c * 48 + tap_b * 8 + (2 - tap_a if flip else tap_a)
        pick = jnp.where((lane == where) & (tap < 27), 1.0, 0.0).astype(BF)
        base = lax.dot_general(
            wrow[...].astype(BF), pick, (((0,), (0,)), ((), ())), preferred_element_type=F32
        )
        for part in range(2):
            for zo in range(4):
                for r in range(2):
                    row = (1 + r) if part == 0 else 3 * r
                    shift = row * 8 + zo
                    moved = base if shift == 0 else pltpu.roll(base, shift, 1)
                    at = part * 512 + flip * 256 + zo * 64 + r * 32
                    w1s[at : at + 32, :] = moved[:, :144].astype(BF)
    nothing = jnp.zeros((CH, 96), F32)
    for a in range(3):
        taps = [w2[3 * a + b].astype(F32) for b in range(3)]
        for ro in range(2):
            pieces = [nothing] + taps if ro else taps + [nothing]
            block = jnp.concatenate(pieces, axis=1).astype(BF)
            for zp in range(2):
                slot = zp - a + 2
                if 0 <= slot < 4:
                    at = (slot * 2 + ro) * 32
                    w2s[at : at + 32, zp * 384 : zp * 384 + 384] = block
    for slot, zp in ((3, 0), (0, 1)):
        w2s[slot * 64 : slot * 64 + 64, zp * 384 : zp * 384 + 384] = jnp.zeros((64, 384), BF)

    oz = offs[0, me]
    rows = iota((48, 384), 0)
    cols = iota((48, 384), 1)
    slot_n = lax.shift_right_logical(cols, 7)
    from_z = lax.shift_right_logical(cols & 127, 1)
    from_row = slot_n * 2 + (cols & 1)
    to_row = lax.shift_right_logical(rows, 3)
    low = jnp.where(sp == 0, 2, 0)
    high = jnp.where(sp == NS - 1, 3, 5)
    keep_row = (from_row == to_row) & (to_row >= low) & (to_row <= high)
    for b in range(4):
        rel = (rows & 7) + (4 * b - 1)
        hit = keep_row & (from_z == rel + oz) & (rel >= 0) & (rel < PZ)
        sels[b * 48 : b * 48 + 48, :] = jnp.where(hit, 1.0, 0.0).astype(BF)

    for n in range(3):
        def wait_image(q, c, n=n):
            image_arrival(n, q).wait_recv()
            return c
        if n == 1:
            lax.fori_loop(1, NP, lambda k, c: wait_image(group(k), c), 0)
        else:
            lax.fori_loop(0, NP, wait_image, 0)

    rowsel = jnp.dot(sels[...], gath[...].reshape(384, PX), preferred_element_type=F32)
    lane_r = iota((192, PX), 1)
    before = jnp.where(lane_r == 0, 0.0, pltpu.roll(rowsel, 1, 1))
    after = jnp.where(lane_r == PX - 1, 0.0, pltpu.roll(rowsel, PX - 1, 1))
    for c, cells in enumerate((before, rowsel, after)):
        for b in range(4):
            cut = cells[b * 48 : b * 48 + 48].astype(BF)
            im2[c * 48 : c * 48 + 48, b * PX : b * PX + PX] = cut
            im2[(2 - c) * 48 : (2 - c) * 48 + 48, 512 + b * PX : 512 + b * PX + PX] = cut

    def sums(parts):
        first = parts[0]
        second = parts[0] * parts[0]
        for part in parts[1:]:
            first = first + part
            second = second + part * part
        return first, second

    def to_lanes(blocks):
        cells = jnp.concatenate(blocks, axis=0)
        return jnp.sum(jnp.transpose(cells), axis=0, keepdims=True)

    own[...] = jnp.dot(w1s[:512], im2[...], preferred_element_type=F32)
    firsts, seconds = [], []
    for zf in range(2):
        for xf in range(2):
            one, two = sums([
                own[zf * 256 + i * 32 : zf * 256 + i * 32 + 32, xf * 512 + b * PX : xf * 512 + b * PX + PX]
                for i in range(8) for b in range(4)
            ])
            firsts.append(one)
            seconds.append(two)

    def stat_copy(buf, ssem, rsem, k):
        return pltpu.make_async_remote_copy(
            src_ref=buf.at[sp], dst_ref=buf.at[sp],
            send_sem=ssem.at[k], recv_sem=rsem.at[sp],
            device_id=(me, space(k)), device_id_type=MESH,
        )

    def stat_arrival(buf, ssem, rsem, k):
        return pltpu.make_async_remote_copy(
            src_ref=buf.at[space(k)], dst_ref=buf.at[space(k)],
            send_sem=ssem.at[k], recv_sem=rsem.at[space(k)],
            device_id=(me, space(k)), device_id_type=MESH,
        )

    def send_stats(buf, ssem, rsem):
        for k in sorted(range(1, NS), key=far):
            stat_copy(buf, ssem, rsem, k).start()

    def wait_stats(buf, ssem, rsem):
        def body(k, c):
            stat_arrival(buf, ssem, rsem, k).wait_recv()
            return c
        lax.fori_loop(1, NS, body, 0)

    def scales(buf, gain, bias):
        total = jnp.sum(buf[...], axis=0)
        cells = float(PZ * PY * PX)
        mean = total[0:1] / cells
        variance = total[1:2] / cells - mean * mean
        factor = lax.rsqrt(variance + 1e-05) * jnp.concatenate([gain[...]] * 4, axis=1)
        shift = jnp.concatenate([bias[...]] * 4, axis=1) - mean * factor
        return (
            jnp.transpose(jnp.broadcast_to(factor, (128, 128))),
            jnp.transpose(jnp.broadcast_to(shift, (128, 128))),
        )

    def leaky(u):
        return jnp.maximum(u, 0.01 * u)

    st1[sp] = jnp.concatenate([to_lanes(firsts), to_lanes(seconds)], axis=0)
    send_stats(st1, s_st1, r_st1)

    halo[...] = jnp.dot(w1s[512:], im2[...], preferred_element_type=F32)

    row16 = iota((16, 512), 0)
    col16 = iota((16, 512), 1)
    head = jnp.concatenate([hw[...].astype(F32)] * 16, axis=1)
    k16 = lax.shift_right_logical(row16 & 7, 1)
    spread = jnp.zeros((16, 512), F32)
    for k in range(3):
        spread = jnp.where(k16 == k, head[k : k + 1, :], spread)
    same = (lax.shift_right_logical(row16, 3) == (lax.shift_right_logical(col16, 6) & 1)) & (
        (row16 & 1) == (lax.shift_right_logical(col16, 5) & 1)
    )
    whs[...] = jnp.where(same, spread, 0.0).astype(BF)

    lead = iota((128, PX), 0)
    width = iota((128, PX), 1)
    row_y = (2 * sp + (lead & 1)).astype(F32)
    wmap[...] = (
        gauss(lax.shift_right_logical(lead, 3).astype(F32), PZ) * gauss(row_y, PY) * gauss(width.astype(F32), PX)
    )

    r48 = iota((48, 128), 0)
    c48 = iota((48, 128), 1)
    z48 = lax.shift_right_logical(r48 * 43, 8)
    m48 = r48 - z48 * 6
    for q in range(NP):
        hit = ((c48 & 7) == m48) & (lax.shift_right_logical(c48, 3) == z48 + 8 * q - oz)
        place[q * 48 : q * 48 + 48, :] = jnp.where(hit, 1.0, 0.0).astype(BF)

    rc = iota((48, VX), 0)
    xc = iota((48, VX), 1)
    zc = lax.shift_right_logical(rc * 43, 8)
    yc = (2 * sp + ((rc - zc * 6) & 1)).astype(F32)
    plane = jnp.zeros((48, VX), F32)
    for p in range(NP):
        rel_z = 8 * me + zc - offs[0, p]
        rel_x = xc - offs[1, p]
        inside = (rel_z >= 0) & (rel_z < PZ) & (rel_x >= 0) & (rel_x < PX)
        value = gauss(rel_z.astype(F32), PZ) * gauss(rel_x.astype(F32), PX)
        plane = plane + jnp.where(inside, value, 0.0)
    inv[...] = jnp.maximum(plane * gauss(yc, PY), 0.1)

    back = iota((PX, VX), 1) - iota((PX, VX), 0)
    for p in range(NP):
        unblend[p * PX : p * PX + PX, :] = jnp.where(back == offs[1, p], 1.0, 0.0).astype(BF)

    wait_stats(st1, s_st1, r_st1)
    factor1, shift1 = scales(st1, g1, b1)

    edge = (jnp.where(sp == 0, 0.0, 1.0), jnp.where(sp == NS - 1, 0.0, 1.0))
    lane_b = iota((CH, PX), 1)
    firsts, seconds = [], []
    for zf in range(2):
        for xf in range(2):
            f = zf * 2 + xf
            scale = factor1[f * 32 : f * 32 + 32]
            shift = shift1[f * 32 : f * 32 + 32]
            for zo in range(4):
                for row in range(4):
                    source = own if row in (1, 2) else halo
                    r = row - 1 if row in (1, 2) else row // 3
                    at = zf * 256 + zo * 64 + r * 32
                    if row in (0, 3):
                        sc, sh = scale * edge[row // 3], shift * edge[row // 3]
                    else:
                        sc, sh = scale, shift
                    zp = zo % 2
                    zi = 1 - zp if zf else zp
                    for b in range(4):
                        j = 2 * b + zo // 2
                        u = leaky(source[at : at + 32, xf * 512 + b * PX : xf * 512 + b * PX + PX] * sc + sh)
                        prior = jnp.where(lane_b == 0, 0.0, pltpu.roll(u, 1, 1))
                        later = jnp.where(lane_b == PX - 1, 0.0, pltpu.roll(u, PX - 1, 1))
                        for c, cells in enumerate((prior, u, later)):
                            ci = 2 - c if xf else c
                            k = ((zi * 4 + row) * 3 + ci) * 32
                            act[k : k + 32, f * 1024 + j * PX : f * 1024 + j * PX + PX] = cells.astype(BF)
            pbuf[...] = jnp.dot(w2s[...], act[:, f * 1024 : f * 1024 + 1024], preferred_element_type=F32)

            def slot(s, j):
                s = 3 - s if zf else s
                return pbuf[s * 64 : s * 64 + 64, j * PX : j * PX + PX]

            parts = []
            for j in range(8):
                even = slot(1, j)
                if j > 0:
                    even = even + slot(3, j - 1)
                odd = slot(2, j)
                if j < 7:
                    odd = odd + slot(0, j + 1)
                for zp, value in enumerate((even, odd)):
                    at = f * 128 + zp * 64
                    conv[at : at + 64, j * PX : j * PX + PX] = value
                    parts.append(value[:32])
                    parts.append(value[32:])
            one, two = sums(parts)
            firsts.append(one)
            seconds.append(two)

    st2[sp] = jnp.concatenate([to_lanes(firsts), to_lanes(seconds)], axis=0)
    send_stats(st2, s_st2, r_st2)
    wait_stats(st2, s_st2, r_st2)
    factor2, shift2 = scales(st2, g2, b2)

    for f in range(4):
        scale = factor2[f * 32 : f * 32 + 32]
        shift = shift2[f * 32 : f * 32 + 32]
        for i in range(4):
            at = f * 128 + i * 32
            for j in range(8):
                u = leaky(conv[at : at + 32, j * PX : j * PX + PX] * scale + shift)
                hid[at : at + 32, j * PX : j * PX + PX] = u.astype(BF)
    raw = jnp.dot(whs[...], hid[...], preferred_element_type=F32)
    k_of = lax.shift_right_logical(iota((16, PX), 0) & 7, 1)
    head_b = jnp.where(k_of == 0, hb[0], jnp.where(k_of == 1, hb[1], hb[2]))
    for j in range(8):
        value = (raw[:, j * PX : j * PX + PX] * 0.25 + head_b) * wmap[j * 16 : j * 16 + 16, :]
        logit[j * 16 : j * 16 + 16, :] = value.astype(BF)
    placed = jnp.dot(place[...], logit[...], preferred_element_type=F32)
    for q in range(NP):
        msend[q] = placed[q * 48 : q * 48 + 48].astype(BF)

    def out_copy(q):
        return pltpu.make_async_remote_copy(
            src_ref=msend.at[q], dst_ref=mrecv.at[me],
            send_sem=s_out.at[q], recv_sem=r_out.at[me],
            device_id=(q, sp), device_id_type=MESH,
        )

    def out_arrival(q):
        return pltpu.make_async_remote_copy(
            src_ref=msend.at[q], dst_ref=mrecv.at[q],
            send_sem=s_out.at[q], recv_sem=r_out.at[q],
            device_id=(q, sp), device_id_type=MESH,
        )

    def send_out(k, c):
        out_copy(group(k)).start()
        return c

    lax.fori_loop(1, NP, send_out, 0)
    mrecv[me] = msend[me]

    def drain_images(k, c):
        image_copy(0, group(k)).wait_send()
        image_copy(2, group(k)).wait_send()
        image_copy(1, group(k)).wait_send()
        return c

    lax.fori_loop(1, NP, drain_images, 0)
    image_copy(0, me).wait_send()
    image_copy(2, me).wait_send()

    def drain_stats(k, c):
        stat_copy(st1, s_st1, r_st1, k).wait_send()
        stat_copy(st2, s_st2, r_st2, k).wait_send()
        return c

    lax.fori_loop(1, NS, drain_stats, 0)

    def drain_out(k, c):
        out_copy(group(k)).wait_send()
        return c

    lax.fori_loop(1, NP, drain_out, 0)

    def wait_out(k, c):
        out_arrival(group(k)).wait_recv()
        return c

    lax.fori_loop(1, NP, wait_out, 0)


def place_kernel(mrecv, unblend, inv, out):
    got = jnp.concatenate([mrecv[p] for p in range(NP)], axis=1)
    final = jnp.dot(got, unblend[...], preferred_element_type=F32) / inv[...]
    for z in range(8):
        for k in range(3):
            out[z, k] = final[z * 6 + k * 2 : z * 6 + k * 2 + 2, :]


def local(image, offsets, w1, w2, g1, b1, g2, b2, hw, hb):
    vm = pl.BlockSpec(memory_space=pltpu.VMEM)
    hold = pl.BlockSpec(memory_space=pltpu.HBM)
    dma = pltpu.SemaphoreType.DMA
    inputs = (
        image, offsets.T, w1.transpose(0, 2, 1), w2, g1.reshape(1, CH), b1.reshape(1, CH), g2.reshape(1, CH),
        b2.reshape(1, CH), hw, hb,
    )
    blocks = pl.pallas_call(
        kernel,
        out_shape=(
            pltpu.VMEM((NP, 48, PX), BF),
            pltpu.VMEM((NP * PX, VX), BF),
            pltpu.VMEM((48, VX), F32),
        ),
        in_specs=[hold] * 10,
        out_specs=(vm, vm, vm),
        scratch_shapes=[
            pltpu.VMEM((8, 2, VX), BF),
            pltpu.SMEM((2, NP), jnp.int32),
            pltpu.VMEM((9, 3, CH), BF),
            pltpu.VMEM((9, CH, 96), BF),
            pltpu.VMEM((1, CH), F32),
            pltpu.VMEM((1, CH), F32),
            pltpu.VMEM((1, CH), F32),
            pltpu.VMEM((1, CH), F32),
            pltpu.VMEM((3, CH), BF),
            pltpu.SMEM((3,), F32),
            pltpu.VMEM((CH, CH), F32),
            pltpu.VMEM((16, VX), F32),
            pltpu.VMEM((NP, 16, PX), BF),
            pltpu.VMEM((3, NP, 16, PX), BF),
            pltpu.VMEM((1024, 144), BF),
            pltpu.VMEM((256, 768), BF),
            pltpu.VMEM((16, 512), BF),
            pltpu.VMEM((192, 384), BF),
            pltpu.VMEM((144, 1024), BF),
            pltpu.VMEM((512, 1024), F32),
            pltpu.VMEM((512, 1024), F32),
            pltpu.VMEM((768, 4096), BF),
            pltpu.VMEM((256, 1024), F32),
            pltpu.VMEM((512, 1024), F32),
            pltpu.VMEM((512, 1024), BF),
            pltpu.VMEM((NS, 2, PX), F32),
            pltpu.VMEM((NS, 2, PX), F32),
            pltpu.VMEM((384, PX), BF),
            pltpu.VMEM((128, PX), F32),
            pltpu.VMEM((128, PX), BF),
            pltpu.VMEM((NP, 48, PX), BF),
            dma((10,)), dma((3, NP)), dma((3, NP)),
            dma((NS,)), dma((NS,)), dma((NS,)), dma((NS,)),
            dma((NP,)), dma((NP,)),
        ],
        compiler_params=pltpu.CompilerParams(
            collective_id=0, has_side_effects=True, vmem_limit_bytes=40 * 1024 * 1024
        ),
    )(*[pltpu.with_memory_space_constraint(value, pltpu.HBM) for value in inputs])
    return pl.pallas_call(
        place_kernel,
        out_shape=jax.ShapeDtypeStruct((8, 3, 2, VX), F32),
        in_specs=[vm, vm, vm],
        out_specs=vm,
        compiler_params=pltpu.CompilerParams(vmem_limit_bytes=8 * 1024 * 1024),
    )(*[pltpu.with_memory_space_constraint(b, pltpu.VMEM) for b in blocks])


def solution(mesh):
    return jax.shard_map(
        local,
        mesh=mesh,
        in_specs=(P("patch", "space", None), P(), P(), P(), P(), P(), P(), P(), P(), P()),
        out_specs=P("patch", None, "space", None),
        check_vma=False,
    )
```

```python
import jax
import jax.numpy as jnp
from jax import lax
from jax.experimental import pallas as pl
from jax.experimental.pallas import tpu as pltpu
from jax.sharding import PartitionSpec as P

PX = 128
PZ = 16
CH = 32
NP = 8
NS = 32
PY = 64
VX = 256
MESH = pl.DeviceIdType.MESH
BF = jnp.bfloat16
F32 = jnp.float32
HI = lax.Precision.HIGHEST


def iota(shape, dim):
    return lax.broadcasted_iota(jnp.int32, shape, dim)


def gauss(positions, length):
    center = (length - 1) / 2.0
    deviation = length / 8.0
    offset = positions - center
    return jnp.exp(-(offset * offset) / (2.0 * deviation * deviation))


def far(k):
    dz = (k + 1) // 4
    return -min(dz, 8 - dz) - min(k % 4, 4 - k % 4)


def kernel(
    image_in, offs_in, w1_in, w2_in, g1_in, b1_in, g2_in, b2_in, hw_in, hb_in, mrecv, unblend, inv,
    image, offs, w1, w2, g1, b1, g2, b2, hw, hb, wrow, slab, xsend, gath, w1s, w2s, whs, sels, im2, own, halo, act, pbuf, conv, hid,
    st1, st2, place, wmap, logit, msend,
    rounds, s_in, s_img, r_img, s_st1, r_st1, s_st2, r_st2, s_out, r_out,
):
    me = lax.axis_index("patch")
    sp = lax.axis_index("space")

    def space(k):
        return lax.rem(sp + k + NS, NS)

    def group(k):
        return lax.rem(me + k, NP)

    barrier = pltpu.get_barrier_semaphore()

    def greet(p, s):
        pl.semaphore_signal(barrier, inc=1, device_id=(p, s), device_id_type=MESH)

    above = sp > 0
    below = sp < NS - 1
    layer, rank = lax.div(sp, 4), lax.rem(sp, 4)

    def torus(dz, dy):
        return lax.rem(layer + dz + 8, 8) * 4 + lax.rem(rank + dy + 4, 4)

    order = (4, 5, 3, 2, 6, 7, 1)

    @pl.when(below)
    def _():
        for k in order + (0,):
            greet(group(k), sp + 1)

    @pl.when(above)
    def _():
        for k in order + (0,):
            greet(group(k), sp - 1)

    for k in order:
        greet(group(k), sp)
    for dz, dy in ((1, 0), (-1, 0), (0, 1), (0, -1)):
        greet(me, torus(dz, dy))

    pairs = (
        (image_in, image), (offs_in, offs), (w1_in, w1), (w2_in, w2), (g1_in, g1),
        (b1_in, b1), (g2_in, g2), (b2_in, b2), (hw_in, hw), (hb_in, hb),
    )
    loads = [pltpu.make_async_copy(src, dst, s_in.at[i]) for i, (src, dst) in enumerate(pairs)]
    for load in loads:
        load.start()
    wrow[...] = jnp.zeros_like(wrow)
    for load in loads[:2]:
        load.wait()

    for z in range(8):
        slab[2 * z : 2 * z + 2, :] = image[z].astype(F32)
    diff = iota((VX, PX), 0) - iota((VX, PX), 1)
    for p in range(NP):
        pick = jnp.where(diff == offs[1, p], 1.0, 0.0).astype(BF)
        xsend[p] = jnp.dot(slab[...].astype(BF), pick, preferred_element_type=F32).astype(BF)

    near = jnp.where(above, NP, 0) + jnp.where(below, NP, 0) + NP - 1 + 4
    pl.semaphore_wait(barrier, near)

    def tell(i, dz, dy):
        for sign in (1, -1):
            pl.semaphore_signal(
                rounds.at[i], inc=1, device_id=(me, torus(sign * dz, sign * dy)), device_id_type=MESH
            )

    tell(0, 0, 1)

    def image_copy(n, p):
        return pltpu.make_async_remote_copy(
            src_ref=xsend.at[p], dst_ref=gath.at[n, me],
            send_sem=s_img.at[n, p], recv_sem=r_img.at[n, me],
            device_id=(p, space(1 - n)), device_id_type=MESH,
        )

    def image_arrival(n, q):
        return pltpu.make_async_remote_copy(
            src_ref=xsend.at[q], dst_ref=gath.at[n, q],
            send_sem=s_img.at[n, q], recv_sem=r_img.at[n, q],
            device_id=(q, space(1 - n)), device_id_type=MESH,
        )

    @pl.when(below)
    def _():
        for k in order + (0,):
            image_copy(0, group(k)).start()

    @pl.when(above)
    def _():
        for k in order + (0,):
            image_copy(2, group(k)).start()

    for k in order:
        image_copy(1, group(k)).start()
    gath[1, me] = xsend[me]

    @pl.when(jnp.logical_not(above))
    def _():
        gath[0] = jnp.zeros_like(gath[0])

    @pl.when(jnp.logical_not(below))
    def _():
        gath[2] = jnp.zeros_like(gath[2])

    for load in loads[2:]:
        load.wait()
    for t in range(9):
        wrow[3 * t : 3 * t + 3, :] = w1[t].astype(F32)
    lane = iota((CH, VX), 1)
    tap = iota((CH, VX), 0)
    tap_a = lax.shift_right_logical(tap * 57, 9)
    tap_r = tap - 9 * tap_a
    tap_b = lax.shift_right_logical(tap_r * 11, 5)
    tap_c = tap_r - 3 * tap_b
    for flip in range(2):
        where = tap_c * 48 + tap_b * 8 + (2 - tap_a if flip else tap_a)
        pick = jnp.where((lane == where) & (tap < 27), 1.0, 0.0).astype(BF)
        base = lax.dot_general(
            wrow[...].astype(BF), pick, (((0,), (0,)), ((), ())), preferred_element_type=F32
        )
        for part in range(2):
            for zo in range(4):
                for r in range(2):
                    row = (1 + r) if part == 0 else 3 * r
                    shift = row * 8 + zo
                    moved = base if shift == 0 else pltpu.roll(base, shift, 1)
                    at = part * 512 + flip * 256 + zo * 64 + r * 32
                    w1s[at : at + 32, :] = moved[:, :144].astype(BF)
    pl.semaphore_wait(rounds.at[0], 2)
    tell(1, 1, 0)
    nothing = jnp.zeros((CH, 96), F32)
    for a in range(3):
        taps = [w2[3 * a + b].astype(F32) for b in range(3)]
        for ro in range(2):
            pieces = [nothing] + taps if ro else taps + [nothing]
            block = jnp.concatenate(pieces, axis=1).astype(BF)
            for zp in range(2):
                slot = zp - a + 2
                if 0 <= slot < 4:
                    at = (slot * 2 + ro) * 32
                    w2s[at : at + 32, zp * 384 : zp * 384 + 384] = block
    for slot, zp in ((3, 0), (0, 1)):
        w2s[slot * 64 : slot * 64 + 64, zp * 384 : zp * 384 + 384] = jnp.zeros((64, 384), BF)

    pl.semaphore_wait(rounds.at[1], 2)
    tell(2, 2, 0)
    pl.semaphore_signal(rounds.at[2], inc=1, device_id=(me, torus(2, 1)), device_id_type=MESH)
    oz = offs[0, me]
    rows = iota((48, 384), 0)
    cols = iota((48, 384), 1)
    slot_n = lax.shift_right_logical(cols, 7)
    from_z = lax.shift_right_logical(cols & 127, 1)
    from_row = slot_n * 2 + (cols & 1)
    to_row = lax.shift_right_logical(rows, 3)
    low = jnp.where(sp == 0, 2, 0)
    high = jnp.where(sp == NS - 1, 3, 5)
    keep_row = (from_row == to_row) & (to_row >= low) & (to_row <= high)
    for b in range(4):
        rel = (rows & 7) + (4 * b - 1)
        hit = keep_row & (from_z == rel + oz) & (rel >= 0) & (rel < PZ)
        sels[b * 48 : b * 48 + 48, :] = jnp.where(hit, 1.0, 0.0).astype(BF)

    def wait_images(n, first):
        def body(k, c):
            image_arrival(n, group(k)).wait_recv()
            return c

        lax.fori_loop(first, NP, body, 0)

    wait_images(1, 1)

    @pl.when(above)
    def _():
        wait_images(0, 0)

    @pl.when(below)
    def _():
        wait_images(2, 0)

    rowsel = jnp.dot(sels[...], gath[...].reshape(384, PX), preferred_element_type=F32)
    lane_r = iota((192, PX), 1)
    before = jnp.where(lane_r == 0, 0.0, pltpu.roll(rowsel, 1, 1))
    after = jnp.where(lane_r == PX - 1, 0.0, pltpu.roll(rowsel, PX - 1, 1))
    for c, cells in enumerate((before, rowsel, after)):
        for b in range(4):
            cut = cells[b * 48 : b * 48 + 48].astype(BF)
            im2[c * 48 : c * 48 + 48, b * PX : b * PX + PX] = cut
            im2[(2 - c) * 48 : (2 - c) * 48 + 48, 512 + b * PX : 512 + b * PX + PX] = cut

    def sums(parts):
        first = parts[0]
        second = parts[0] * parts[0]
        for part in parts[1:]:
            first = first + part
            second = second + part * part
        return first, second

    def to_lanes(blocks):
        cells = jnp.concatenate(blocks, axis=0)
        return jnp.sum(jnp.transpose(cells), axis=0, keepdims=True)

    own[...] = jnp.dot(w1s[:512], im2[...], preferred_element_type=F32)
    firsts, seconds = [], []
    for zf in range(2):
        for xf in range(2):
            one, two = sums([
                own[zf * 256 + i * 32 : zf * 256 + i * 32 + 32, xf * 512 + b * PX : xf * 512 + b * PX + PX]
                for i in range(8) for b in range(4)
            ])
            firsts.append(one)
            seconds.append(two)

    def stat_copy(buf, ssem, rsem, k):
        return pltpu.make_async_remote_copy(
            src_ref=buf.at[sp], dst_ref=buf.at[sp],
            send_sem=ssem.at[k], recv_sem=rsem.at[sp],
            device_id=(me, space(k)), device_id_type=MESH,
        )

    def stat_arrival(buf, ssem, rsem, k):
        return pltpu.make_async_remote_copy(
            src_ref=buf.at[space(k)], dst_ref=buf.at[space(k)],
            send_sem=ssem.at[k], recv_sem=rsem.at[space(k)],
            device_id=(me, space(k)), device_id_type=MESH,
        )

    def send_stats(buf, ssem, rsem):
        for k in sorted(range(1, NS), key=far):
            stat_copy(buf, ssem, rsem, k).start()

    def wait_stats(buf, ssem, rsem):
        def body(k, c):
            stat_arrival(buf, ssem, rsem, k).wait_recv()
            return c
        lax.fori_loop(1, NS, body, 0)

    def scales(buf, gain, bias):
        total = jnp.sum(buf[...], axis=0)
        cells = float(PZ * PY * PX)
        mean = total[0:1] / cells
        variance = total[1:2] / cells - mean * mean
        factor = lax.rsqrt(variance + 1e-05) * jnp.concatenate([gain[...]] * 4, axis=1)
        shift = jnp.concatenate([bias[...]] * 4, axis=1) - mean * factor
        return (
            jnp.transpose(jnp.broadcast_to(factor, (128, 128))),
            jnp.transpose(jnp.broadcast_to(shift, (128, 128))),
        )

    def leaky(u):
        return jnp.maximum(u, 0.01 * u)

    st1[sp] = jnp.concatenate([to_lanes(firsts), to_lanes(seconds)], axis=0)
    pl.semaphore_wait(rounds.at[2], 3)
    send_stats(st1, s_st1, r_st1)

    halo[...] = jnp.dot(w1s[512:], im2[...], preferred_element_type=F32)

    row16 = iota((16, 512), 0)
    col16 = iota((16, 512), 1)
    head = jnp.concatenate([hw[...].astype(F32)] * 16, axis=1)
    k16 = lax.shift_right_logical(row16 & 7, 1)
    spread = jnp.zeros((16, 512), F32)
    for k in range(3):
        spread = jnp.where(k16 == k, head[k : k + 1, :], spread)
    same = (lax.shift_right_logical(row16, 3) == (lax.shift_right_logical(col16, 6) & 1)) & (
        (row16 & 1) == (lax.shift_right_logical(col16, 5) & 1)
    )
    whs[...] = jnp.where(same, spread, 0.0).astype(BF)

    lead = iota((128, PX), 0)
    width = iota((128, PX), 1)
    row_y = (2 * sp + (lead & 1)).astype(F32)
    wmap[...] = (
        gauss(lax.shift_right_logical(lead, 3).astype(F32), PZ) * gauss(row_y, PY) * gauss(width.astype(F32), PX)
    )

    r48 = iota((48, 128), 0)
    c48 = iota((48, 128), 1)
    z48 = lax.shift_right_logical(r48 * 43, 8)
    m48 = r48 - z48 * 6
    for q in range(NP):
        hit = ((c48 & 7) == m48) & (lax.shift_right_logical(c48, 3) == z48 + 8 * q - oz)
        place[q * 48 : q * 48 + 48, :] = jnp.where(hit, 1.0, 0.0).astype(BF)

    rc = iota((48, VX), 0)
    xc = iota((48, VX), 1)
    zc = lax.shift_right_logical(rc * 43, 8)
    yc = (2 * sp + ((rc - zc * 6) & 1)).astype(F32)
    plane = jnp.zeros((48, VX), F32)
    for p in range(NP):
        rel_z = 8 * me + zc - offs[0, p]
        rel_x = xc - offs[1, p]
        inside = (rel_z >= 0) & (rel_z < PZ) & (rel_x >= 0) & (rel_x < PX)
        value = gauss(rel_z.astype(F32), PZ) * gauss(rel_x.astype(F32), PX)
        plane = plane + jnp.where(inside, value, 0.0)
    inv[...] = jnp.maximum(plane * gauss(yc, PY), 0.1)

    back = iota((PX, VX), 1) - iota((PX, VX), 0)
    for p in range(NP):
        unblend[p * PX : p * PX + PX, :] = jnp.where(back == offs[1, p], 1.0, 0.0).astype(BF)

    wait_stats(st1, s_st1, r_st1)
    factor1, shift1 = scales(st1, g1, b1)

    edge = (jnp.where(sp == 0, 0.0, 1.0), jnp.where(sp == NS - 1, 0.0, 1.0))
    lane_b = iota((CH, PX), 1)
    firsts, seconds = [], []
    for zf in range(2):
        for xf in range(2):
            f = zf * 2 + xf
            scale = factor1[f * 32 : f * 32 + 32]
            shift = shift1[f * 32 : f * 32 + 32]
            for zo in range(4):
                for row in range(4):
                    source = own if row in (1, 2) else halo
                    r = row - 1 if row in (1, 2) else row // 3
                    at = zf * 256 + zo * 64 + r * 32
                    if row in (0, 3):
                        sc, sh = scale * edge[row // 3], shift * edge[row // 3]
                    else:
                        sc, sh = scale, shift
                    zp = zo % 2
                    zi = 1 - zp if zf else zp
                    for b in range(4):
                        j = 2 * b + zo // 2
                        u = leaky(source[at : at + 32, xf * 512 + b * PX : xf * 512 + b * PX + PX] * sc + sh)
                        prior = jnp.where(lane_b == 0, 0.0, pltpu.roll(u, 1, 1))
                        later = jnp.where(lane_b == PX - 1, 0.0, pltpu.roll(u, PX - 1, 1))
                        for c, cells in enumerate((prior, u, later)):
                            ci = 2 - c if xf else c
                            k = ((zi * 4 + row) * 3 + ci) * 32
                            act[k : k + 32, f * 1024 + j * PX : f * 1024 + j * PX + PX] = cells.astype(BF)
            pbuf[...] = jnp.dot(w2s[...], act[:, f * 1024 : f * 1024 + 1024], preferred_element_type=F32)

            def slot(s, j):
                s = 3 - s if zf else s
                return pbuf[s * 64 : s * 64 + 64, j * PX : j * PX + PX]

            parts = []
            for j in range(8):
                even = slot(1, j)
                if j > 0:
                    even = even + slot(3, j - 1)
                odd = slot(2, j)
                if j < 7:
                    odd = odd + slot(0, j + 1)
                for zp, value in enumerate((even, odd)):
                    at = f * 128 + zp * 64
                    conv[at : at + 64, j * PX : j * PX + PX] = value
                    parts.append(value[:32])
                    parts.append(value[32:])
            one, two = sums(parts)
            firsts.append(one)
            seconds.append(two)

    st2[sp] = jnp.concatenate([to_lanes(firsts), to_lanes(seconds)], axis=0)
    send_stats(st2, s_st2, r_st2)
    wait_stats(st2, s_st2, r_st2)
    factor2, shift2 = scales(st2, g2, b2)

    for f in range(4):
        scale = factor2[f * 32 : f * 32 + 32]
        shift = shift2[f * 32 : f * 32 + 32]
        for i in range(4):
            at = f * 128 + i * 32
            for j in range(8):
                u = leaky(conv[at : at + 32, j * PX : j * PX + PX] * scale + shift)
                hid[at : at + 32, j * PX : j * PX + PX] = u.astype(BF)
    raw = jnp.dot(whs[...], hid[...], preferred_element_type=F32)
    k_of = lax.shift_right_logical(iota((16, PX), 0) & 7, 1)
    head_b = jnp.where(k_of == 0, hb[0], jnp.where(k_of == 1, hb[1], hb[2]))
    for j in range(8):
        value = (raw[:, j * PX : j * PX + PX] * 0.25 + head_b) * wmap[j * 16 : j * 16 + 16, :]
        logit[j * 16 : j * 16 + 16, :] = value.astype(BF)
    placed = jnp.dot(place[...], logit[...], preferred_element_type=F32)
    for q in range(NP):
        msend[q] = placed[q * 48 : q * 48 + 48].astype(BF)

    def out_copy(q):
        return pltpu.make_async_remote_copy(
            src_ref=msend.at[q], dst_ref=mrecv.at[me],
            send_sem=s_out.at[q], recv_sem=r_out.at[me],
            device_id=(q, sp), device_id_type=MESH,
        )

    def out_arrival(q):
        return pltpu.make_async_remote_copy(
            src_ref=msend.at[q], dst_ref=mrecv.at[q],
            send_sem=s_out.at[q], recv_sem=r_out.at[q],
            device_id=(q, sp), device_id_type=MESH,
        )

    def send_out(k, c):
        out_copy(group(k)).start()
        return c

    lax.fori_loop(1, NP, send_out, 0)
    mrecv[me] = msend[me]

    def drain_images(n, first):
        def body(k, c):
            image_copy(n, group(k)).wait_send()
            return c

        lax.fori_loop(first, NP, body, 0)

    drain_images(1, 1)

    @pl.when(below)
    def _():
        drain_images(0, 0)

    @pl.when(above)
    def _():
        drain_images(2, 0)

    def drain_stats(k, c):
        stat_copy(st1, s_st1, r_st1, k).wait_send()
        stat_copy(st2, s_st2, r_st2, k).wait_send()
        return c

    lax.fori_loop(1, NS, drain_stats, 0)

    def drain_out(k, c):
        out_copy(group(k)).wait_send()
        return c

    lax.fori_loop(1, NP, drain_out, 0)

    def wait_out(k, c):
        out_arrival(group(k)).wait_recv()
        return c

    lax.fori_loop(1, NP, wait_out, 0)


def place_kernel(mrecv, unblend, inv, out):
    got = jnp.concatenate([mrecv[p] for p in range(NP)], axis=1)
    final = jnp.dot(got, unblend[...], preferred_element_type=F32) / inv[...]
    for z in range(8):
        for k in range(3):
            out[z, k] = final[z * 6 + k * 2 : z * 6 + k * 2 + 2, :]


def local(image, offsets, w1, w2, g1, b1, g2, b2, hw, hb):
    vm = pl.BlockSpec(memory_space=pltpu.VMEM)
    hold = pl.BlockSpec(memory_space=pltpu.HBM)
    dma = pltpu.SemaphoreType.DMA
    inputs = (
        image, offsets.T, w1.transpose(0, 2, 1), w2, g1.reshape(1, CH), b1.reshape(1, CH), g2.reshape(1, CH),
        b2.reshape(1, CH), hw, hb,
    )
    blocks = pl.pallas_call(
        kernel,
        out_shape=(
            pltpu.VMEM((NP, 48, PX), BF),
            pltpu.VMEM((NP * PX, VX), BF),
            pltpu.VMEM((48, VX), F32),
        ),
        in_specs=[hold] * 10,
        out_specs=(vm, vm, vm),
        scratch_shapes=[
            pltpu.VMEM((8, 2, VX), BF),
            pltpu.SMEM((2, NP), jnp.int32),
            pltpu.VMEM((9, 3, CH), BF),
            pltpu.VMEM((9, CH, 96), BF),
            pltpu.VMEM((1, CH), F32),
            pltpu.VMEM((1, CH), F32),
            pltpu.VMEM((1, CH), F32),
            pltpu.VMEM((1, CH), F32),
            pltpu.VMEM((3, CH), BF),
            pltpu.SMEM((3,), F32),
            pltpu.VMEM((CH, CH), F32),
            pltpu.VMEM((16, VX), F32),
            pltpu.VMEM((NP, 16, PX), BF),
            pltpu.VMEM((3, NP, 16, PX), BF),
            pltpu.VMEM((1024, 144), BF),
            pltpu.VMEM((256, 768), BF),
            pltpu.VMEM((16, 512), BF),
            pltpu.VMEM((192, 384), BF),
            pltpu.VMEM((144, 1024), BF),
            pltpu.VMEM((512, 1024), F32),
            pltpu.VMEM((512, 1024), F32),
            pltpu.VMEM((768, 4096), BF),
            pltpu.VMEM((256, 1024), F32),
            pltpu.VMEM((512, 1024), F32),
            pltpu.VMEM((512, 1024), BF),
            pltpu.VMEM((NS, 2, PX), F32),
            pltpu.VMEM((NS, 2, PX), F32),
            pltpu.VMEM((384, PX), BF),
            pltpu.VMEM((128, PX), F32),
            pltpu.VMEM((128, PX), BF),
            pltpu.VMEM((NP, 48, PX), BF),
            pltpu.SemaphoreType.REGULAR((3,)),
            dma((10,)), dma((3, NP)), dma((3, NP)),
            dma((NS,)), dma((NS,)), dma((NS,)), dma((NS,)),
            dma((NP,)), dma((NP,)),
        ],
        compiler_params=pltpu.CompilerParams(
            collective_id=0, has_side_effects=True, vmem_limit_bytes=40 * 1024 * 1024
        ),
    )(*[pltpu.with_memory_space_constraint(value, pltpu.HBM) for value in inputs])
    return pl.pallas_call(
        place_kernel,
        out_shape=jax.ShapeDtypeStruct((8, 3, 2, VX), F32),
        in_specs=[vm, vm, vm],
        out_specs=vm,
        compiler_params=pltpu.CompilerParams(vmem_limit_bytes=8 * 1024 * 1024),
    )(*[pltpu.with_memory_space_constraint(b, pltpu.VMEM) for b in blocks])


def solution(mesh):
    return jax.shard_map(
        local,
        mesh=mesh,
        in_specs=(P("patch", "space", None), P(), P(), P(), P(), P(), P(), P(), P(), P()),
        out_specs=P("patch", None, "space", None),
        check_vma=False,
    )
```

```python
import jax
import jax.numpy as jnp
from jax import lax
from jax.experimental import pallas as pl
from jax.experimental.pallas import tpu as pltpu
from jax.sharding import PartitionSpec as P

PX = 128
PZ = 16
CH = 32
NP = 8
NS = 32
PY = 64
VX = 256
MESH = pl.DeviceIdType.MESH
BF = jnp.bfloat16
F32 = jnp.float32
HI = lax.Precision.HIGHEST


def iota(shape, dim):
    return lax.broadcasted_iota(jnp.int32, shape, dim)


def wide(ref, blocks):
    return jnp.concatenate([ref[i] for i in blocks], axis=1)


def gauss(positions, length):
    center = (length - 1) / 2.0
    deviation = length / 8.0
    offset = positions - center
    return jnp.exp(-(offset * offset) / (2.0 * deviation * deviation))


def far(k):
    dz = (k + 1) // 4
    return -min(dz, 8 - dz) - min(k % 4, 4 - k % 4)


def kernel(
    image_in, offs_in, w1_in, w2_in, g1_in, b1_in, g2_in, b2_in, hw_in, hb_in, mrecv, unblend, inv,
    image, offs, w1, w2, g1, b1, g2, b2, hw, hb, wrow, slab, xsend, gath, w1s, w2s, whs, sels, im2, own, halo, act, pbuf, conv, hid,
    st1, st2, place, wmap, logit, msend,
    late, s_in, s_img, r_img, s_st1, r_st1, s_st2, r_st2, s_out, r_out,
):
    me = lax.axis_index("patch")
    sp = lax.axis_index("space")

    def space(k):
        return lax.rem(sp + k + NS, NS)

    def group(k):
        return lax.rem(me + k, NP)

    barrier = pltpu.get_barrier_semaphore()

    def greet(p, s):
        pl.semaphore_signal(barrier, inc=1, device_id=(p, s), device_id_type=MESH)

    above = sp > 0
    below = sp < NS - 1
    layer, rank = lax.div(sp, 4), lax.rem(sp, 4)

    def torus(dz, dy):
        return lax.rem(layer + dz + 8, 8) * 4 + lax.rem(rank + dy + 4, 4)

    order = (4, 5, 3, 2, 6, 7, 1)

    @pl.when(below)
    def _():
        for k in order + (0,):
            greet(group(k), sp + 1)

    @pl.when(above)
    def _():
        for k in order + (0,):
            greet(group(k), sp - 1)

    for k in order:
        greet(group(k), sp)
    def release(dz, dy):
        z = lax.rem(layer + dz + 8, 8)
        y = lax.rem(rank + dy + 4, 4)
        return jnp.minimum(z, 4) + jnp.minimum(y, 4 - y)

    mine = release(0, 0)
    others = sorted(
        ((dz, dy) for dz in range(-3, 5) for dy in range(-1, 3) if (dz, dy) != (0, 0)),
        key=lambda d: -abs(d[0]) - abs(d[1]),
    )

    def tell(signal, later):
        for dz, dy in others:
            theirs = release(dz, dy)

            @pl.when(theirs >= mine if later else theirs < mine)
            def _(dz=dz, dy=dy):
                pl.semaphore_signal(signal, inc=1, device_id=(me, torus(dz, dy)), device_id_type=MESH)

    tell(barrier, True)
    known = 0
    for at, count in enumerate((1, 4, 8, 12, 19, 28, 32)):
        known = jnp.where(mine == at, count, known)

    pairs = (
        (image_in, image), (offs_in, offs), (w1_in, w1), (w2_in, w2), (g1_in, g1),
        (b1_in, b1), (g2_in, g2), (b2_in, b2), (hw_in, hw), (hb_in, hb),
    )
    loads = [pltpu.make_async_copy(src, dst, s_in.at[i]) for i, (src, dst) in enumerate(pairs)]
    for load in loads:
        load.start()
    wrow[...] = jnp.zeros_like(wrow)
    for load in loads[:2]:
        load.wait()

    for z in range(8):
        slab[2 * z : 2 * z + 2, :] = image[z].astype(F32)
    diff = iota((VX, PX), 0) - iota((VX, PX), 1)
    for p in range(NP):
        pick = jnp.where(diff == offs[1, p], 1.0, 0.0).astype(BF)
        xsend[p] = jnp.dot(slab[...].astype(BF), pick, preferred_element_type=F32).astype(BF)

    near = jnp.where(above, NP, 0) + jnp.where(below, NP, 0) + NP - 1
    pl.semaphore_wait(barrier, near + known - 1)

    def image_copy(n, p):
        return pltpu.make_async_remote_copy(
            src_ref=xsend.at[p], dst_ref=gath.at[n, me],
            send_sem=s_img.at[n, p], recv_sem=r_img.at[n, me],
            device_id=(p, space(1 - n)), device_id_type=MESH,
        )

    def image_arrival(n, q):
        return pltpu.make_async_remote_copy(
            src_ref=xsend.at[q], dst_ref=gath.at[n, q],
            send_sem=s_img.at[n, q], recv_sem=r_img.at[n, q],
            device_id=(q, space(1 - n)), device_id_type=MESH,
        )

    @pl.when(below)
    def _():
        for k in order + (0,):
            image_copy(0, group(k)).start()

    @pl.when(above)
    def _():
        for k in order + (0,):
            image_copy(2, group(k)).start()

    for k in order:
        image_copy(1, group(k)).start()
    tell(late, False)
    gath[1, me] = xsend[me]

    @pl.when(jnp.logical_not(above))
    def _():
        gath[0] = jnp.zeros_like(gath[0])

    @pl.when(jnp.logical_not(below))
    def _():
        gath[2] = jnp.zeros_like(gath[2])

    for load in loads[2:]:
        load.wait()
    for t in range(9):
        wrow[3 * t : 3 * t + 3, :] = w1[t].astype(F32)
    lane = iota((CH, VX), 1)
    tap = iota((CH, VX), 0)
    tap_a = lax.shift_right_logical(tap * 57, 9)
    tap_r = tap - 9 * tap_a
    tap_b = lax.shift_right_logical(tap_r * 11, 5)
    tap_c = tap_r - 3 * tap_b
    for flip in range(2):
        where = tap_c * 48 + tap_b * 8 + (2 - tap_a if flip else tap_a)
        pick = jnp.where((lane == where) & (tap < 27), 1.0, 0.0).astype(BF)
        base = lax.dot_general(
            wrow[...].astype(BF), pick, (((0,), (0,)), ((), ())), preferred_element_type=F32
        )
        for part in range(2):
            for zo in range(4):
                for r in range(2):
                    row = (1 + r) if part == 0 else 3 * r
                    shift = row * 8 + zo
                    moved = base if shift == 0 else pltpu.roll(base, shift, 1)
                    at = part * 512 + flip * 256 + zo * 64 + r * 32
                    w1s[at : at + 32, :] = moved[:, :144].astype(BF)
    nothing = jnp.zeros((CH, 96), F32)
    for a in range(3):
        taps = [w2[3 * a + b].astype(F32) for b in range(3)]
        for ro in range(2):
            pieces = [nothing] + taps if ro else taps + [nothing]
            block = jnp.concatenate(pieces, axis=1).astype(BF)
            for zp in range(2):
                slot = zp - a + 2
                if 0 <= slot < 4:
                    at = (slot * 2 + ro) * 32
                    for i in range(3):
                        w2s[zp * 3 + i, at : at + 32, :] = block[:, i * PX : i * PX + PX]
    for slot, zp in ((3, 0), (0, 1)):
        for i in range(3):
            w2s[zp * 3 + i, slot * 64 : slot * 64 + 64, :] = jnp.zeros((64, PX), BF)

    oz = offs[0, me]
    rows = iota((48, 384), 0)
    cols = iota((48, 384), 1)
    slot_n = lax.shift_right_logical(cols, 7)
    from_z = lax.shift_right_logical(cols & 127, 1)
    from_row = slot_n * 2 + (cols & 1)
    to_row = lax.shift_right_logical(rows, 3)
    low = jnp.where(sp == 0, 2, 0)
    high = jnp.where(sp == NS - 1, 3, 5)
    keep_row = (from_row == to_row) & (to_row >= low) & (to_row <= high)
    for b in range(4):
        rel = (rows & 7) + (4 * b - 1)
        hit = keep_row & (from_z == rel + oz) & (rel >= 0) & (rel < PZ)
        sels[b * 48 : b * 48 + 48, :] = jnp.where(hit, 1.0, 0.0).astype(BF)

    def wait_images(n, first):
        def body(k, c):
            image_arrival(n, group(k)).wait_recv()
            return c

        lax.fori_loop(first, NP, body, 0)

    wait_images(1, 1)

    @pl.when(above)
    def _():
        wait_images(0, 0)

    @pl.when(below)
    def _():
        wait_images(2, 0)

    rowsel = jnp.dot(sels[...], gath[...].reshape(384, PX), preferred_element_type=F32)
    lane_r = iota((192, PX), 1)
    before = jnp.where(lane_r == 0, 0.0, pltpu.roll(rowsel, 1, 1))
    after = jnp.where(lane_r == PX - 1, 0.0, pltpu.roll(rowsel, PX - 1, 1))
    for c, cells in enumerate((before, rowsel, after)):
        for b in range(4):
            cut = cells[b * 48 : b * 48 + 48].astype(BF)
            im2[b, c * 48 : c * 48 + 48, :] = cut
            im2[4 + b, (2 - c) * 48 : (2 - c) * 48 + 48, :] = cut

    def sums(parts):
        first = parts[0]
        second = parts[0] * parts[0]
        for part in parts[1:]:
            first = first + part
            second = second + part * part
        return first, second

    def to_lanes(blocks):
        cells = jnp.concatenate(blocks, axis=0)
        return jnp.sum(jnp.transpose(cells), axis=0, keepdims=True)

    own[...] = jnp.dot(w1s[:512], wide(im2, range(8)), preferred_element_type=F32)
    firsts, seconds = [], []
    for zf in range(2):
        for xf in range(2):
            one, two = sums([
                own[zf * 256 + i * 32 : zf * 256 + i * 32 + 32, xf * 512 + b * PX : xf * 512 + b * PX + PX]
                for i in range(8) for b in range(4)
            ])
            firsts.append(one)
            seconds.append(two)

    def stat_copy(buf, ssem, rsem, k):
        return pltpu.make_async_remote_copy(
            src_ref=buf.at[sp], dst_ref=buf.at[sp],
            send_sem=ssem.at[k], recv_sem=rsem.at[sp],
            device_id=(me, space(k)), device_id_type=MESH,
        )

    def stat_arrival(buf, ssem, rsem, k):
        return pltpu.make_async_remote_copy(
            src_ref=buf.at[space(k)], dst_ref=buf.at[space(k)],
            send_sem=ssem.at[k], recv_sem=rsem.at[space(k)],
            device_id=(me, space(k)), device_id_type=MESH,
        )

    def send_stats(buf, ssem, rsem):
        for k in sorted(range(1, NS), key=far):
            stat_copy(buf, ssem, rsem, k).start()

    def wait_stats(buf, ssem, rsem):
        def body(k, c):
            stat_arrival(buf, ssem, rsem, k).wait_recv()
            return c
        lax.fori_loop(1, NS, body, 0)

    def scales(buf, gain, bias):
        total = jnp.sum(buf[...], axis=0)
        cells = float(PZ * PY * PX)
        mean = total[0:1] / cells
        variance = total[1:2] / cells - mean * mean
        factor = lax.rsqrt(variance + 1e-05) * jnp.concatenate([gain[...]] * 4, axis=1)
        shift = jnp.concatenate([bias[...]] * 4, axis=1) - mean * factor
        return (
            jnp.transpose(jnp.broadcast_to(factor, (128, 128))),
            jnp.transpose(jnp.broadcast_to(shift, (128, 128))),
        )

    def leaky(u):
        return jnp.maximum(u, 0.01 * u)

    st1[sp] = jnp.concatenate([to_lanes(firsts), to_lanes(seconds)], axis=0)
    @pl.when(known < NS)
    def _():
        pl.semaphore_wait(late, NS - known)

    send_stats(st1, s_st1, r_st1)

    halo[...] = jnp.dot(w1s[512:], wide(im2, range(8)), preferred_element_type=F32)

    row16 = iota((16, 512), 0)
    col16 = iota((16, 512), 1)
    head = jnp.concatenate([hw[...].astype(F32)] * 16, axis=1)
    k16 = lax.shift_right_logical(row16 & 7, 1)
    spread = jnp.zeros((16, 512), F32)
    for k in range(3):
        spread = jnp.where(k16 == k, head[k : k + 1, :], spread)
    same = (lax.shift_right_logical(row16, 3) == (lax.shift_right_logical(col16, 6) & 1)) & (
        (row16 & 1) == (lax.shift_right_logical(col16, 5) & 1)
    )
    whs[...] = jnp.where(same, spread, 0.0).astype(BF)

    lead = iota((128, PX), 0)
    width = iota((128, PX), 1)
    row_y = (2 * sp + (lead & 1)).astype(F32)
    wmap[...] = (
        gauss(lax.shift_right_logical(lead, 3).astype(F32), PZ) * gauss(row_y, PY) * gauss(width.astype(F32), PX)
    )

    r48 = iota((48, 128), 0)
    c48 = iota((48, 128), 1)
    z48 = lax.shift_right_logical(r48 * 43, 8)
    m48 = r48 - z48 * 6
    for q in range(NP):
        hit = ((c48 & 7) == m48) & (lax.shift_right_logical(c48, 3) == z48 + 8 * q - oz)
        place[q * 48 : q * 48 + 48, :] = jnp.where(hit, 1.0, 0.0).astype(BF)

    rc = iota((48, VX), 0)
    xc = iota((48, VX), 1)
    zc = lax.shift_right_logical(rc * 43, 8)
    yc = (2 * sp + ((rc - zc * 6) & 1)).astype(F32)
    plane = jnp.zeros((48, VX), F32)
    for p in range(NP):
        rel_z = 8 * me + zc - offs[0, p]
        rel_x = xc - offs[1, p]
        inside = (rel_z >= 0) & (rel_z < PZ) & (rel_x >= 0) & (rel_x < PX)
        value = gauss(rel_z.astype(F32), PZ) * gauss(rel_x.astype(F32), PX)
        plane = plane + jnp.where(inside, value, 0.0)
    inv[...] = jnp.maximum(plane * gauss(yc, PY), 0.1)

    back = iota((PX, VX), 1) - iota((PX, VX), 0)
    for p in range(NP):
        unblend[p * PX : p * PX + PX, :] = jnp.where(back == offs[1, p], 1.0, 0.0).astype(BF)

    wait_stats(st1, s_st1, r_st1)
    factor1, shift1 = scales(st1, g1, b1)

    edge = (jnp.where(sp == 0, 0.0, 1.0), jnp.where(sp == NS - 1, 0.0, 1.0))
    lane_b = iota((CH, PX), 1)
    zero_b = jnp.zeros((CH, PX), BF)
    firsts, seconds = [], []
    for zf in range(2):
        for xf in range(2):
            f = zf * 2 + xf
            scale = factor1[f * 32 : f * 32 + 32]
            shift = shift1[f * 32 : f * 32 + 32]
            for zo in range(4):
                for row in range(4):
                    source = own if row in (1, 2) else halo
                    r = row - 1 if row in (1, 2) else row // 3
                    at = zf * 256 + zo * 64 + r * 32
                    if row in (0, 3):
                        sc, sh = scale * edge[row // 3], shift * edge[row // 3]
                    else:
                        sc, sh = scale, shift
                    zp = zo % 2
                    zi = 1 - zp if zf else zp
                    for b in range(4):
                        j = 2 * b + zo // 2
                        u = leaky(source[at : at + 32, xf * 512 + b * PX : xf * 512 + b * PX + PX] * sc + sh)
                        u = u.astype(BF)
                        prior = jnp.where(lane_b == 0, zero_b, pltpu.roll(u, 1, 1))
                        later = jnp.where(lane_b == PX - 1, zero_b, pltpu.roll(u, PX - 1, 1))
                        for c, cells in enumerate((prior, u, later)):
                            ci = 2 - c if xf else c
                            k = ((zi * 4 + row) * 3 + ci) * 32
                            act[f * 8 + j, k : k + 32, :] = cells
            pbuf[...] = jnp.dot(
                wide(w2s, range(6)), wide(act, range(f * 8, f * 8 + 8)), preferred_element_type=F32
            )

            def slot(s, j):
                s = 3 - s if zf else s
                return pbuf[s * 64 : s * 64 + 64, j * PX : j * PX + PX]

            parts = []
            for j in range(8):
                even = slot(1, j)
                if j > 0:
                    even = even + slot(3, j - 1)
                odd = slot(2, j)
                if j < 7:
                    odd = odd + slot(0, j + 1)
                for zp, value in enumerate((even, odd)):
                    at = f * 128 + zp * 64
                    conv[at : at + 64, j * PX : j * PX + PX] = value
                    parts.append(value[:32])
                    parts.append(value[32:])
            one, two = sums(parts)
            firsts.append(one)
            seconds.append(two)

    st2[sp] = jnp.concatenate([to_lanes(firsts), to_lanes(seconds)], axis=0)
    send_stats(st2, s_st2, r_st2)
    wait_stats(st2, s_st2, r_st2)
    factor2, shift2 = scales(st2, g2, b2)

    for f in range(4):
        scale = factor2[f * 32 : f * 32 + 32]
        shift = shift2[f * 32 : f * 32 + 32]
        for i in range(4):
            at = f * 128 + i * 32
            for j in range(8):
                u = leaky(conv[at : at + 32, j * PX : j * PX + PX] * scale + shift)
                hid[j, at : at + 32, :] = u.astype(BF)
    raw = jnp.dot(whs[...], wide(hid, range(8)), preferred_element_type=F32)
    k_of = lax.shift_right_logical(iota((16, PX), 0) & 7, 1)
    head_b = jnp.where(k_of == 0, hb[0], jnp.where(k_of == 1, hb[1], hb[2]))
    for j in range(8):
        value = (raw[:, j * PX : j * PX + PX] * 0.25 + head_b) * wmap[j * 16 : j * 16 + 16, :]
        logit[j * 16 : j * 16 + 16, :] = value.astype(BF)
    placed = jnp.dot(place[...], logit[...], preferred_element_type=F32)
    for q in range(NP):
        msend[q] = placed[q * 48 : q * 48 + 48].astype(BF)

    def out_copy(q):
        return pltpu.make_async_remote_copy(
            src_ref=msend.at[q], dst_ref=mrecv.at[me],
            send_sem=s_out.at[q], recv_sem=r_out.at[me],
            device_id=(q, sp), device_id_type=MESH,
        )

    def out_arrival(q):
        return pltpu.make_async_remote_copy(
            src_ref=msend.at[q], dst_ref=mrecv.at[q],
            send_sem=s_out.at[q], recv_sem=r_out.at[q],
            device_id=(q, sp), device_id_type=MESH,
        )

    def send_out(k, c):
        out_copy(group(k)).start()
        return c

    lax.fori_loop(1, NP, send_out, 0)
    mrecv[me] = msend[me]

    def drain_images(n, first):
        def body(k, c):
            image_copy(n, group(k)).wait_send()
            return c

        lax.fori_loop(first, NP, body, 0)

    drain_images(1, 1)

    @pl.when(below)
    def _():
        drain_images(0, 0)

    @pl.when(above)
    def _():
        drain_images(2, 0)

    def drain_stats(k, c):
        stat_copy(st1, s_st1, r_st1, k).wait_send()
        stat_copy(st2, s_st2, r_st2, k).wait_send()
        return c

    lax.fori_loop(1, NS, drain_stats, 0)

    def drain_out(k, c):
        out_copy(group(k)).wait_send()
        return c

    lax.fori_loop(1, NP, drain_out, 0)

    def wait_out(k, c):
        out_arrival(group(k)).wait_recv()
        return c

    lax.fori_loop(1, NP, wait_out, 0)


def place_kernel(mrecv, unblend, inv, out):
    got = jnp.concatenate([mrecv[p] for p in range(NP)], axis=1)
    final = jnp.dot(got, unblend[...], preferred_element_type=F32) / inv[...]
    for z in range(8):
        for k in range(3):
            out[z, k] = final[z * 6 + k * 2 : z * 6 + k * 2 + 2, :]


def local(image, offsets, w1, w2, g1, b1, g2, b2, hw, hb):
    vm = pl.BlockSpec(memory_space=pltpu.VMEM)
    hold = pl.BlockSpec(memory_space=pltpu.HBM)
    dma = pltpu.SemaphoreType.DMA
    inputs = (
        image, offsets.T, w1.transpose(0, 2, 1), w2, g1.reshape(1, CH), b1.reshape(1, CH), g2.reshape(1, CH),
        b2.reshape(1, CH), hw, hb,
    )
    blocks = pl.pallas_call(
        kernel,
        out_shape=(
            pltpu.VMEM((NP, 48, PX), BF),
            pltpu.VMEM((NP * PX, VX), BF),
            pltpu.VMEM((48, VX), F32),
        ),
        in_specs=[hold] * 10,
        out_specs=(vm, vm, vm),
        scratch_shapes=[
            pltpu.VMEM((8, 2, VX), BF),
            pltpu.SMEM((2, NP), jnp.int32),
            pltpu.VMEM((9, 3, CH), BF),
            pltpu.VMEM((9, CH, 96), BF),
            pltpu.VMEM((1, CH), F32),
            pltpu.VMEM((1, CH), F32),
            pltpu.VMEM((1, CH), F32),
            pltpu.VMEM((1, CH), F32),
            pltpu.VMEM((3, CH), BF),
            pltpu.SMEM((3,), F32),
            pltpu.VMEM((CH, CH), F32),
            pltpu.VMEM((16, VX), F32),
            pltpu.VMEM((NP, 16, PX), BF),
            pltpu.VMEM((3, NP, 16, PX), BF),
            pltpu.VMEM((1024, 144), BF),
            pltpu.VMEM((6, 256, PX), BF),
            pltpu.VMEM((16, 512), BF),
            pltpu.VMEM((192, 384), BF),
            pltpu.VMEM((8, 144, PX), BF),
            pltpu.VMEM((512, 1024), F32),
            pltpu.VMEM((512, 1024), F32),
            pltpu.VMEM((32, 768, PX), BF),
            pltpu.VMEM((256, 1024), F32),
            pltpu.VMEM((512, 1024), F32),
            pltpu.VMEM((8, 512, PX), BF),
            pltpu.VMEM((NS, 2, PX), F32),
            pltpu.VMEM((NS, 2, PX), F32),
            pltpu.VMEM((384, PX), BF),
            pltpu.VMEM((128, PX), F32),
            pltpu.VMEM((128, PX), BF),
            pltpu.VMEM((NP, 48, PX), BF),
            pltpu.SemaphoreType.REGULAR,
            dma((10,)), dma((3, NP)), dma((3, NP)),
            dma((NS,)), dma((NS,)), dma((NS,)), dma((NS,)),
            dma((NP,)), dma((NP,)),
        ],
        compiler_params=pltpu.CompilerParams(
            collective_id=0, has_side_effects=True, vmem_limit_bytes=40 * 1024 * 1024
        ),
    )(*[pltpu.with_memory_space_constraint(value, pltpu.HBM) for value in inputs])
    return pl.pallas_call(
        place_kernel,
        out_shape=jax.ShapeDtypeStruct((8, 3, 2, VX), F32),
        in_specs=[vm, vm, vm],
        out_specs=vm,
        compiler_params=pltpu.CompilerParams(vmem_limit_bytes=8 * 1024 * 1024),
    )(*[pltpu.with_memory_space_constraint(b, pltpu.VMEM) for b in blocks])


def solution(mesh):
    return jax.shard_map(
        local,
        mesh=mesh,
        in_specs=(P("patch", "space", None), P(), P(), P(), P(), P(), P(), P(), P(), P()),
        out_specs=P("patch", None, "space", None),
        check_vma=False,
    )
```

```python
import jax
import jax.numpy as jnp
from jax import lax
from jax.experimental import pallas as pl
from jax.experimental.pallas import tpu as pltpu
from jax.sharding import PartitionSpec as P

PX = 128
PZ = 16
CH = 32
NP = 8
NS = 32
PY = 64
VX = 256
MESH = pl.DeviceIdType.MESH
BF = jnp.bfloat16
F32 = jnp.float32
HI = lax.Precision.HIGHEST


def iota(shape, dim):
    return lax.broadcasted_iota(jnp.int32, shape, dim)


def wide(ref, blocks):
    return jnp.concatenate([ref[i] for i in blocks], axis=1)


def gauss(positions, length):
    center = (length - 1) / 2.0
    deviation = length / 8.0
    offset = positions - center
    return jnp.exp(-(offset * offset) / (2.0 * deviation * deviation))


def far(k):
    dz = (k + 1) // 4
    return -min(dz, 8 - dz) - min(k % 4, 4 - k % 4)


def kernel(
    image_in, offs_in, w1_in, w2_in, g1_in, b1_in, g2_in, b2_in, hw_in, hb_in, mrecv, unblend, inv,
    image, offs, w1, w2, g1, b1, g2, b2, hw, hb, wrow, slab, xsend, gath, w1s, w2s, whs, sels, im2, own, halo, act, pbuf, conv, hid,
    st1, st2, place, wmap, logit, msend,
    late, late_x, s_in, s_img, r_img, s_st1, r_st1, s_st2, r_st2, s_out, r_out,
):
    me = lax.axis_index("patch")
    sp = lax.axis_index("space")

    def space(k):
        return lax.rem(sp + k + NS, NS)

    def group(k):
        return lax.rem(me + k, NP)

    barrier = pltpu.get_barrier_semaphore()

    def greet(p, s):
        pl.semaphore_signal(barrier, inc=1, device_id=(p, s), device_id_type=MESH)

    above = sp > 0
    below = sp < NS - 1
    layer, rank = lax.div(sp, 4), lax.rem(sp, 4)

    def torus(dz, dy):
        return lax.rem(layer + dz + 8, 8) * 4 + lax.rem(rank + dy + 4, 4)

    order = (4, 5, 3, 2, 6, 7, 1)

    def column(k):
        x = lax.div(group(k), 2)
        return jnp.minimum(x, 4 - x)

    mine_x = column(0)
    seen = jnp.where(mine_x == 0, 2, jnp.where(mine_x == 1, 6, 8))
    blocks = 1 + jnp.where(above, 1, 0) + jnp.where(below, 1, 0)

    def tell_columns(signal, later):
        for k in order + (0,):
            theirs = column(k)

            @pl.when(theirs >= mine_x if later else theirs < mine_x)
            def _(k=k):
                def one(s):
                    pl.semaphore_signal(signal, inc=1, device_id=(group(k), s), device_id_type=MESH)

                @pl.when(below)
                def _():
                    one(sp + 1)

                @pl.when(above)
                def _():
                    one(sp - 1)

                if k:
                    one(sp)

    tell_columns(barrier, True)

    def release(dz, dy):
        z = lax.rem(layer + dz + 8, 8)
        y = lax.rem(rank + dy + 4, 4)
        return jnp.minimum(z, 4) + jnp.minimum(y, 4 - y)

    mine = release(0, 0)
    others = sorted(
        ((dz, dy) for dz in range(-3, 5) for dy in range(-1, 3) if (dz, dy) != (0, 0)),
        key=lambda d: -abs(d[0]) - abs(d[1]),
    )

    def tell(signal, later):
        for dz, dy in others:
            theirs = release(dz, dy)

            @pl.when(theirs >= mine if later else theirs < mine)
            def _(dz=dz, dy=dy):
                pl.semaphore_signal(signal, inc=1, device_id=(me, torus(dz, dy)), device_id_type=MESH)

    tell(barrier, True)
    known = 0
    for at, count in enumerate((1, 4, 8, 12, 19, 28, 32)):
        known = jnp.where(mine == at, count, known)

    pairs = (
        (image_in, image), (offs_in, offs), (w1_in, w1), (w2_in, w2), (g1_in, g1),
        (b1_in, b1), (g2_in, g2), (b2_in, b2), (hw_in, hw), (hb_in, hb),
    )
    loads = [pltpu.make_async_copy(src, dst, s_in.at[i]) for i, (src, dst) in enumerate(pairs)]
    for load in loads:
        load.start()
    wrow[...] = jnp.zeros_like(wrow)
    for load in loads[:2]:
        load.wait()

    for z in range(8):
        slab[2 * z : 2 * z + 2, :] = image[z].astype(F32)
    diff = iota((VX, PX), 0) - iota((VX, PX), 1)
    for p in range(NP):
        pick = jnp.where(diff == offs[1, p], 1.0, 0.0).astype(BF)
        xsend[p] = jnp.dot(slab[...].astype(BF), pick, preferred_element_type=F32).astype(BF)

    pl.semaphore_wait(barrier, seen * blocks - 1 + known - 1)
    tell_columns(late_x, False)
    tell(late, False)

    def image_copy(n, p):
        return pltpu.make_async_remote_copy(
            src_ref=xsend.at[p], dst_ref=gath.at[n, me],
            send_sem=s_img.at[n, p], recv_sem=r_img.at[n, me],
            device_id=(p, space(1 - n)), device_id_type=MESH,
        )

    def image_arrival(n, q):
        return pltpu.make_async_remote_copy(
            src_ref=xsend.at[q], dst_ref=gath.at[n, q],
            send_sem=s_img.at[n, q], recv_sem=r_img.at[n, q],
            device_id=(q, space(1 - n)), device_id_type=MESH,
        )

    def send_images(known_first):
        for k in order + (0,):
            theirs = column(k)

            @pl.when(theirs <= mine_x if known_first else theirs > mine_x)
            def _(k=k):
                @pl.when(below)
                def _():
                    image_copy(0, group(k)).start()

                @pl.when(above)
                def _():
                    image_copy(2, group(k)).start()

                if k:
                    image_copy(1, group(k)).start()

    send_images(True)

    @pl.when(seen < NP)
    def _():
        pl.semaphore_wait(late_x, (NP - seen) * blocks)
        send_images(False)

    gath[1, me] = xsend[me]

    @pl.when(jnp.logical_not(above))
    def _():
        gath[0] = jnp.zeros_like(gath[0])

    @pl.when(jnp.logical_not(below))
    def _():
        gath[2] = jnp.zeros_like(gath[2])

    for load in loads[2:]:
        load.wait()
    for t in range(9):
        wrow[3 * t : 3 * t + 3, :] = w1[t].astype(F32)
    lane = iota((CH, VX), 1)
    tap = iota((CH, VX), 0)
    tap_a = lax.shift_right_logical(tap * 57, 9)
    tap_r = tap - 9 * tap_a
    tap_b = lax.shift_right_logical(tap_r * 11, 5)
    tap_c = tap_r - 3 * tap_b
    for flip in range(2):
        where = tap_c * 48 + tap_b * 8 + (2 - tap_a if flip else tap_a)
        pick = jnp.where((lane == where) & (tap < 27), 1.0, 0.0).astype(BF)
        base = lax.dot_general(
            wrow[...].astype(BF), pick, (((0,), (0,)), ((), ())), preferred_element_type=F32
        )
        for part in range(2):
            for zo in range(4):
                for r in range(2):
                    row = (1 + r) if part == 0 else 3 * r
                    shift = row * 8 + zo
                    moved = base if shift == 0 else pltpu.roll(base, shift, 1)
                    at = part * 512 + flip * 256 + zo * 64 + r * 32
                    w1s[at : at + 32, :] = moved[:, :144].astype(BF)
    nothing = jnp.zeros((CH, 96), F32)
    for a in range(3):
        taps = [w2[3 * a + b].astype(F32) for b in range(3)]
        for ro in range(2):
            pieces = [nothing] + taps if ro else taps + [nothing]
            block = jnp.concatenate(pieces, axis=1).astype(BF)
            for zp in range(2):
                slot = zp - a + 2
                if 0 <= slot < 4:
                    at = (slot * 2 + ro) * 32
                    for i in range(3):
                        w2s[zp * 3 + i, at : at + 32, :] = block[:, i * PX : i * PX + PX]
    for slot, zp in ((3, 0), (0, 1)):
        for i in range(3):
            w2s[zp * 3 + i, slot * 64 : slot * 64 + 64, :] = jnp.zeros((64, PX), BF)

    oz = offs[0, me]
    rows = iota((48, 384), 0)
    cols = iota((48, 384), 1)
    slot_n = lax.shift_right_logical(cols, 7)
    from_z = lax.shift_right_logical(cols & 127, 1)
    from_row = slot_n * 2 + (cols & 1)
    to_row = lax.shift_right_logical(rows, 3)
    low = jnp.where(sp == 0, 2, 0)
    high = jnp.where(sp == NS - 1, 3, 5)
    keep_row = (from_row == to_row) & (to_row >= low) & (to_row <= high)
    for b in range(4):
        rel = (rows & 7) + (4 * b - 1)
        hit = keep_row & (from_z == rel + oz) & (rel >= 0) & (rel < PZ)
        sels[b * 48 : b * 48 + 48, :] = jnp.where(hit, 1.0, 0.0).astype(BF)

    def wait_images(n, first):
        def body(k, c):
            image_arrival(n, group(k)).wait_recv()
            return c

        lax.fori_loop(first, NP, body, 0)

    wait_images(1, 1)

    @pl.when(above)
    def _():
        wait_images(0, 0)

    @pl.when(below)
    def _():
        wait_images(2, 0)

    rowsel = jnp.dot(sels[...], gath[...].reshape(384, PX), preferred_element_type=F32)
    lane_r = iota((192, PX), 1)
    before = jnp.where(lane_r == 0, 0.0, pltpu.roll(rowsel, 1, 1))
    after = jnp.where(lane_r == PX - 1, 0.0, pltpu.roll(rowsel, PX - 1, 1))
    for c, cells in enumerate((before, rowsel, after)):
        for b in range(4):
            cut = cells[b * 48 : b * 48 + 48].astype(BF)
            im2[b, c * 48 : c * 48 + 48, :] = cut
            im2[4 + b, (2 - c) * 48 : (2 - c) * 48 + 48, :] = cut

    def sums(parts):
        first = parts[0]
        second = parts[0] * parts[0]
        for part in parts[1:]:
            first = first + part
            second = second + part * part
        return first, second

    def to_lanes(blocks):
        cells = jnp.concatenate(blocks, axis=0)
        return jnp.sum(jnp.transpose(cells), axis=0, keepdims=True)

    own[...] = jnp.dot(w1s[:512], wide(im2, range(8)), preferred_element_type=F32)
    firsts, seconds = [], []
    for zf in range(2):
        for xf in range(2):
            one, two = sums([
                own[zf * 256 + i * 32 : zf * 256 + i * 32 + 32, xf * 512 + b * PX : xf * 512 + b * PX + PX]
                for i in range(8) for b in range(4)
            ])
            firsts.append(one)
            seconds.append(two)

    def stat_copy(buf, ssem, rsem, k):
        return pltpu.make_async_remote_copy(
            src_ref=buf.at[sp], dst_ref=buf.at[sp],
            send_sem=ssem.at[k], recv_sem=rsem.at[sp],
            device_id=(me, space(k)), device_id_type=MESH,
        )

    def stat_arrival(buf, ssem, rsem, k):
        return pltpu.make_async_remote_copy(
            src_ref=buf.at[space(k)], dst_ref=buf.at[space(k)],
            send_sem=ssem.at[k], recv_sem=rsem.at[space(k)],
            device_id=(me, space(k)), device_id_type=MESH,
        )

    def send_stats(buf, ssem, rsem):
        for k in sorted(range(1, NS), key=far):
            stat_copy(buf, ssem, rsem, k).start()

    def wait_stats(buf, ssem, rsem):
        for k in sorted(range(1, NS), key=far, reverse=True):
            stat_arrival(buf, ssem, rsem, k).wait_recv()

    def scales(buf, gain, bias):
        total = jnp.sum(buf[...], axis=0)
        cells = float(PZ * PY * PX)
        mean = total[0:1] / cells
        variance = total[1:2] / cells - mean * mean
        factor = lax.rsqrt(variance + 1e-05) * jnp.concatenate([gain[...]] * 4, axis=1)
        shift = jnp.concatenate([bias[...]] * 4, axis=1) - mean * factor
        return (
            jnp.transpose(jnp.broadcast_to(factor, (128, 128))),
            jnp.transpose(jnp.broadcast_to(shift, (128, 128))),
        )

    def leaky(u):
        return jnp.maximum(u, 0.01 * u)

    st1[sp] = jnp.concatenate([to_lanes(firsts), to_lanes(seconds)], axis=0)
    @pl.when(known < NS)
    def _():
        pl.semaphore_wait(late, NS - known)

    send_stats(st1, s_st1, r_st1)

    halo[...] = jnp.dot(w1s[512:], wide(im2, range(8)), preferred_element_type=F32)

    row16 = iota((16, 512), 0)
    col16 = iota((16, 512), 1)
    head = jnp.concatenate([hw[...].astype(F32)] * 16, axis=1)
    k16 = lax.shift_right_logical(row16 & 7, 1)
    spread = jnp.zeros((16, 512), F32)
    for k in range(3):
        spread = jnp.where(k16 == k, head[k : k + 1, :], spread)
    same = (lax.shift_right_logical(row16, 3) == (lax.shift_right_logical(col16, 6) & 1)) & (
        (row16 & 1) == (lax.shift_right_logical(col16, 5) & 1)
    )
    whs[...] = jnp.where(same, spread, 0.0).astype(BF)

    lead = iota((128, PX), 0)
    width = iota((128, PX), 1)
    row_y = (2 * sp + (lead & 1)).astype(F32)
    wmap[...] = (
        gauss(lax.shift_right_logical(lead, 3).astype(F32), PZ) * gauss(row_y, PY) * gauss(width.astype(F32), PX)
    )

    r48 = iota((48, 128), 0)
    c48 = iota((48, 128), 1)
    z48 = lax.shift_right_logical(r48 * 43, 8)
    m48 = r48 - z48 * 6
    for q in range(NP):
        hit = ((c48 & 7) == m48) & (lax.shift_right_logical(c48, 3) == z48 + 8 * q - oz)
        place[q * 48 : q * 48 + 48, :] = jnp.where(hit, 1.0, 0.0).astype(BF)

    rc = iota((48, VX), 0)
    xc = iota((48, VX), 1)
    zc = lax.shift_right_logical(rc * 43, 8)
    yc = (2 * sp + ((rc - zc * 6) & 1)).astype(F32)
    plane = jnp.zeros((48, VX), F32)
    for p in range(NP):
        rel_z = 8 * me + zc - offs[0, p]
        rel_x = xc - offs[1, p]
        inside = (rel_z >= 0) & (rel_z < PZ) & (rel_x >= 0) & (rel_x < PX)
        value = gauss(rel_z.astype(F32), PZ) * gauss(rel_x.astype(F32), PX)
        plane = plane + jnp.where(inside, value, 0.0)
    inv[...] = jnp.maximum(plane * gauss(yc, PY), 0.1)

    back = iota((PX, VX), 1) - iota((PX, VX), 0)
    for p in range(NP):
        unblend[p * PX : p * PX + PX, :] = jnp.where(back == offs[1, p], 1.0, 0.0).astype(BF)

    wait_stats(st1, s_st1, r_st1)
    factor1, shift1 = scales(st1, g1, b1)

    edge = (jnp.where(sp == 0, 0.0, 1.0), jnp.where(sp == NS - 1, 0.0, 1.0))
    lane_b = iota((CH, PX), 1)
    zero_b = jnp.zeros((CH, PX), BF)
    firsts, seconds = [], []
    for zf in range(2):
        for xf in range(2):
            f = zf * 2 + xf
            scale = factor1[f * 32 : f * 32 + 32]
            shift = shift1[f * 32 : f * 32 + 32]
            for zo in range(4):
                for row in range(4):
                    source = own if row in (1, 2) else halo
                    r = row - 1 if row in (1, 2) else row // 3
                    at = zf * 256 + zo * 64 + r * 32
                    if row in (0, 3):
                        sc, sh = scale * edge[row // 3], shift * edge[row // 3]
                    else:
                        sc, sh = scale, shift
                    zp = zo % 2
                    zi = 1 - zp if zf else zp
                    for b in range(4):
                        j = 2 * b + zo // 2
                        u = leaky(source[at : at + 32, xf * 512 + b * PX : xf * 512 + b * PX + PX] * sc + sh)
                        u = u.astype(BF)
                        prior = jnp.where(lane_b == 0, zero_b, pltpu.roll(u, 1, 1))
                        later = jnp.where(lane_b == PX - 1, zero_b, pltpu.roll(u, PX - 1, 1))
                        for c, cells in enumerate((prior, u, later)):
                            ci = 2 - c if xf else c
                            k = ((zi * 4 + row) * 3 + ci) * 32
                            act[f * 8 + j, k : k + 32, :] = cells
            pbuf[...] = jnp.dot(
                wide(w2s, range(6)), wide(act, range(f * 8, f * 8 + 8)), preferred_element_type=F32
            )

            def slot(s, j):
                s = 3 - s if zf else s
                return pbuf[s * 64 : s * 64 + 64, j * PX : j * PX + PX]

            parts = []
            for j in range(8):
                even = slot(1, j)
                if j > 0:
                    even = even + slot(3, j - 1)
                odd = slot(2, j)
                if j < 7:
                    odd = odd + slot(0, j + 1)
                for zp, value in enumerate((even, odd)):
                    at = f * 128 + zp * 64
                    conv[at : at + 64, j * PX : j * PX + PX] = value
                    parts.append(value[:32])
                    parts.append(value[32:])
            one, two = sums(parts)
            firsts.append(one)
            seconds.append(two)

    st2[sp] = jnp.concatenate([to_lanes(firsts), to_lanes(seconds)], axis=0)
    send_stats(st2, s_st2, r_st2)
    wait_stats(st2, s_st2, r_st2)
    factor2, shift2 = scales(st2, g2, b2)

    for f in range(4):
        scale = factor2[f * 32 : f * 32 + 32]
        shift = shift2[f * 32 : f * 32 + 32]
        for i in range(4):
            at = f * 128 + i * 32
            for j in range(8):
                u = leaky(conv[at : at + 32, j * PX : j * PX + PX] * scale + shift)
                hid[j, at : at + 32, :] = u.astype(BF)
    raw = jnp.dot(whs[...], wide(hid, range(8)), preferred_element_type=F32)
    k_of = lax.shift_right_logical(iota((16, PX), 0) & 7, 1)
    head_b = jnp.where(k_of == 0, hb[0], jnp.where(k_of == 1, hb[1], hb[2]))
    for j in range(8):
        value = (raw[:, j * PX : j * PX + PX] * 0.25 + head_b) * wmap[j * 16 : j * 16 + 16, :]
        logit[j * 16 : j * 16 + 16, :] = value.astype(BF)
    placed = jnp.dot(place[...], logit[...], preferred_element_type=F32)
    for q in range(NP):
        msend[q] = placed[q * 48 : q * 48 + 48].astype(BF)

    def out_copy(q):
        return pltpu.make_async_remote_copy(
            src_ref=msend.at[q], dst_ref=mrecv.at[me],
            send_sem=s_out.at[q], recv_sem=r_out.at[me],
            device_id=(q, sp), device_id_type=MESH,
        )

    def out_arrival(q):
        return pltpu.make_async_remote_copy(
            src_ref=msend.at[q], dst_ref=mrecv.at[q],
            send_sem=s_out.at[q], recv_sem=r_out.at[q],
            device_id=(q, sp), device_id_type=MESH,
        )

    def send_out(k, c):
        out_copy(group(k)).start()
        return c

    lax.fori_loop(1, NP, send_out, 0)
    mrecv[me] = msend[me]

    def drain_images(n, first):
        def body(k, c):
            image_copy(n, group(k)).wait_send()
            return c

        lax.fori_loop(first, NP, body, 0)

    drain_images(1, 1)

    @pl.when(below)
    def _():
        drain_images(0, 0)

    @pl.when(above)
    def _():
        drain_images(2, 0)

    def drain_stats(k, c):
        stat_copy(st1, s_st1, r_st1, k).wait_send()
        stat_copy(st2, s_st2, r_st2, k).wait_send()
        return c

    lax.fori_loop(1, NS, drain_stats, 0)

    def drain_out(k, c):
        out_copy(group(k)).wait_send()
        return c

    lax.fori_loop(1, NP, drain_out, 0)

    def wait_out(k, c):
        out_arrival(group(k)).wait_recv()
        return c

    lax.fori_loop(1, NP, wait_out, 0)


def place_kernel(mrecv, unblend, inv, out):
    got = jnp.concatenate([mrecv[p] for p in range(NP)], axis=1)
    final = jnp.dot(got, unblend[...], preferred_element_type=F32) / inv[...]
    for z in range(8):
        for k in range(3):
            out[z, k] = final[z * 6 + k * 2 : z * 6 + k * 2 + 2, :]


def local(image, offsets, w1, w2, g1, b1, g2, b2, hw, hb):
    vm = pl.BlockSpec(memory_space=pltpu.VMEM)
    hold = pl.BlockSpec(memory_space=pltpu.HBM)
    dma = pltpu.SemaphoreType.DMA
    inputs = (
        image, offsets.T, w1.transpose(0, 2, 1), w2, g1.reshape(1, CH), b1.reshape(1, CH), g2.reshape(1, CH),
        b2.reshape(1, CH), hw, hb,
    )
    blocks = pl.pallas_call(
        kernel,
        out_shape=(
            pltpu.VMEM((NP, 48, PX), BF),
            pltpu.VMEM((NP * PX, VX), BF),
            pltpu.VMEM((48, VX), F32),
        ),
        in_specs=[hold] * 10,
        out_specs=(vm, vm, vm),
        scratch_shapes=[
            pltpu.VMEM((8, 2, VX), BF),
            pltpu.SMEM((2, NP), jnp.int32),
            pltpu.VMEM((9, 3, CH), BF),
            pltpu.VMEM((9, CH, 96), BF),
            pltpu.VMEM((1, CH), F32),
            pltpu.VMEM((1, CH), F32),
            pltpu.VMEM((1, CH), F32),
            pltpu.VMEM((1, CH), F32),
            pltpu.VMEM((3, CH), BF),
            pltpu.SMEM((3,), F32),
            pltpu.VMEM((CH, CH), F32),
            pltpu.VMEM((16, VX), F32),
            pltpu.VMEM((NP, 16, PX), BF),
            pltpu.VMEM((3, NP, 16, PX), BF),
            pltpu.VMEM((1024, 144), BF),
            pltpu.VMEM((6, 256, PX), BF),
            pltpu.VMEM((16, 512), BF),
            pltpu.VMEM((192, 384), BF),
            pltpu.VMEM((8, 144, PX), BF),
            pltpu.VMEM((512, 1024), F32),
            pltpu.VMEM((512, 1024), F32),
            pltpu.VMEM((32, 768, PX), BF),
            pltpu.VMEM((256, 1024), F32),
            pltpu.VMEM((512, 1024), F32),
            pltpu.VMEM((8, 512, PX), BF),
            pltpu.VMEM((NS, 2, PX), F32),
            pltpu.VMEM((NS, 2, PX), F32),
            pltpu.VMEM((384, PX), BF),
            pltpu.VMEM((128, PX), F32),
            pltpu.VMEM((128, PX), BF),
            pltpu.VMEM((NP, 48, PX), BF),
            pltpu.SemaphoreType.REGULAR,
            pltpu.SemaphoreType.REGULAR,
            dma((10,)), dma((3, NP)), dma((3, NP)),
            dma((NS,)), dma((NS,)), dma((NS,)), dma((NS,)),
            dma((NP,)), dma((NP,)),
        ],
        compiler_params=pltpu.CompilerParams(
            collective_id=0, has_side_effects=True, vmem_limit_bytes=40 * 1024 * 1024
        ),
    )(*[pltpu.with_memory_space_constraint(value, pltpu.HBM) for value in inputs])
    return pl.pallas_call(
        place_kernel,
        out_shape=jax.ShapeDtypeStruct((8, 3, 2, VX), F32),
        in_specs=[vm, vm, vm],
        out_specs=vm,
        compiler_params=pltpu.CompilerParams(vmem_limit_bytes=8 * 1024 * 1024),
    )(*[pltpu.with_memory_space_constraint(b, pltpu.VMEM) for b in blocks])


def solution(mesh):
    return jax.shard_map(
        local,
        mesh=mesh,
        in_specs=(P("patch", "space", None), P(), P(), P(), P(), P(), P(), P(), P(), P()),
        out_specs=P("patch", None, "space", None),
        check_vma=False,
    )
```

```python
import jax
import jax.numpy as jnp
from jax import lax
from jax.experimental import pallas as pl
from jax.experimental.pallas import tpu as pltpu
from jax.sharding import PartitionSpec as P

PX = 128
PZ = 16
CH = 32
NP = 8
NS = 32
PY = 64
VX = 256
MESH = pl.DeviceIdType.MESH
BF = jnp.bfloat16
F32 = jnp.float32
HI = lax.Precision.HIGHEST


def iota(shape, dim):
    return lax.broadcasted_iota(jnp.int32, shape, dim)


def wide(ref, blocks):
    return jnp.concatenate([ref[i] for i in blocks], axis=1)


def gauss(positions, length):
    center = (length - 1) / 2.0
    deviation = length / 8.0
    offset = positions - center
    return jnp.exp(-(offset * offset) / (2.0 * deviation * deviation))


def far(k):
    dz = (k + 1) // 4
    return -min(dz, 8 - dz) - min(k % 4, 4 - k % 4)


def kernel(
    image_in, offs_in, w1_in, w2_in, g1_in, b1_in, g2_in, b2_in, hw_in, hb_in, mrecv, unblend, inv,
    image, offs, w1, w2, g1, b1, g2, b2, hw, hb, wrow, slab, xsend, gath, w1s, w2s, whs, sels, im2, own, halo, act, pone, ptwo, pbuf, conv, hid,
    st1, st2, place, wmap, logit, msend,
    late, s_in, s_img, r_img, s_st1, r_st1, s_st2, r_st2, s_out, r_out,
):
    me = lax.axis_index("patch")
    sp = lax.axis_index("space")

    def space(k):
        return lax.rem(sp + k + NS, NS)

    def group(k):
        return lax.rem(me + k, NP)

    barrier = pltpu.get_barrier_semaphore()

    def greet(p, s):
        pl.semaphore_signal(barrier, inc=1, device_id=(p, s), device_id_type=MESH)

    above = sp > 0
    below = sp < NS - 1
    layer, rank = lax.div(sp, 4), lax.rem(sp, 4)

    def torus(dz, dy):
        return lax.rem(layer + dz + 8, 8) * 4 + lax.rem(rank + dy + 4, 4)

    order = (4, 5, 3, 2, 6, 7, 1)

    @pl.when(below)
    def _():
        for k in order + (0,):
            greet(group(k), sp + 1)

    @pl.when(above)
    def _():
        for k in order + (0,):
            greet(group(k), sp - 1)

    for k in order:
        greet(group(k), sp)
    def release(dz, dy):
        z = lax.rem(layer + dz + 8, 8)
        y = lax.rem(rank + dy + 4, 4)
        return jnp.minimum(z, 4) + jnp.minimum(y, 4 - y)

    mine = release(0, 0)
    others = sorted(
        ((dz, dy) for dz in range(-3, 5) for dy in range(-1, 3) if (dz, dy) != (0, 0)),
        key=lambda d: -abs(d[0]) - abs(d[1]),
    )

    def tell(signal, later, members):
        for dz, dy in members:
            theirs = release(dz, dy)

            @pl.when(theirs >= mine if later else theirs < mine)
            def _(dz=dz, dy=dy):
                pl.semaphore_signal(signal, inc=1, device_id=(me, torus(dz, dy)), device_id_type=MESH)

    tell(barrier, True, others)
    known = 0
    for at, count in enumerate((1, 4, 8, 12, 19, 28, 32)):
        known = jnp.where(mine == at, count, known)

    pairs = (
        (image_in, image), (offs_in, offs), (w1_in, w1), (w2_in, w2), (g1_in, g1),
        (b1_in, b1), (g2_in, g2), (b2_in, b2), (hw_in, hw), (hb_in, hb),
    )
    loads = [pltpu.make_async_copy(src, dst, s_in.at[i]) for i, (src, dst) in enumerate(pairs)]
    for load in loads:
        load.start()
    wrow[...] = jnp.zeros_like(wrow)
    for load in loads[:2]:
        load.wait()

    for z in range(8):
        slab[2 * z : 2 * z + 2, :] = image[z].astype(F32)
    diff = iota((VX, PX), 0) - iota((VX, PX), 1)
    for p in range(NP):
        pick = jnp.where(diff == offs[1, p], 1.0, 0.0).astype(BF)
        xsend[p] = jnp.dot(slab[...].astype(BF), pick, preferred_element_type=F32).astype(BF)

    near = jnp.where(above, NP, 0) + jnp.where(below, NP, 0) + NP - 1
    pl.semaphore_wait(barrier, near + known - 1)
    tell(late, False, others[:12])

    def image_copy(n, p):
        return pltpu.make_async_remote_copy(
            src_ref=xsend.at[p], dst_ref=gath.at[n, me],
            send_sem=s_img.at[n, p], recv_sem=r_img.at[n, me],
            device_id=(p, space(1 - n)), device_id_type=MESH,
        )

    def image_arrival(n, q):
        return pltpu.make_async_remote_copy(
            src_ref=xsend.at[q], dst_ref=gath.at[n, q],
            send_sem=s_img.at[n, q], recv_sem=r_img.at[n, q],
            device_id=(q, space(1 - n)), device_id_type=MESH,
        )

    @pl.when(below)
    def _():
        for k in order + (0,):
            image_copy(0, group(k)).start()

    @pl.when(above)
    def _():
        for k in order + (0,):
            image_copy(2, group(k)).start()

    for k in order:
        image_copy(1, group(k)).start()
    tell(late, False, others[12:])
    gath[1, me] = xsend[me]

    @pl.when(jnp.logical_not(above))
    def _():
        gath[0] = jnp.zeros_like(gath[0])

    @pl.when(jnp.logical_not(below))
    def _():
        gath[2] = jnp.zeros_like(gath[2])

    for load in loads[2:]:
        load.wait()
    for t in range(9):
        wrow[3 * t : 3 * t + 3, :] = w1[t].astype(F32)
    lane = iota((CH, VX), 1)
    tap = iota((CH, VX), 0)
    tap_a = lax.shift_right_logical(tap * 57, 9)
    tap_r = tap - 9 * tap_a
    tap_b = lax.shift_right_logical(tap_r * 11, 5)
    tap_c = tap_r - 3 * tap_b
    for flip in range(2):
        where = tap_c * 48 + tap_b * 8 + (2 - tap_a if flip else tap_a)
        pick = jnp.where((lane == where) & (tap < 27), 1.0, 0.0).astype(BF)
        base = lax.dot_general(
            wrow[...].astype(BF), pick, (((0,), (0,)), ((), ())), preferred_element_type=F32
        )
        for part in range(2):
            for zo in range(4):
                for r in range(2):
                    row = (1 + r) if part == 0 else 3 * r
                    shift = row * 8 + zo
                    moved = base if shift == 0 else pltpu.roll(base, shift, 1)
                    at = part * 512 + flip * 256 + zo * 64 + r * 32
                    w1s[at : at + 32, :] = moved[:, :144].astype(BF)
    nothing = jnp.zeros((CH, 96), F32)
    for a in range(3):
        taps = [w2[3 * a + b].astype(F32) for b in range(3)]
        for ro in range(2):
            pieces = [nothing] + taps if ro else taps + [nothing]
            pair = jnp.concatenate([piece[:, :64] for piece in pieces], axis=1).astype(BF)
            last = jnp.concatenate([piece[:, 64:] for piece in pieces], axis=1).astype(BF)
            for zp in range(2):
                slot = zp - a + 2
                if 0 <= slot < 4:
                    at = (slot * 2 + ro) * 32
                    for i in range(2):
                        w2s[zp * 2 + i, at : at + 32, :] = pair[:, i * PX : i * PX + PX]
                    w2s[4 + zp, at : at + 32, :] = last
    for slot, zp in ((3, 0), (0, 1)):
        w2s[4 + zp, slot * 64 : slot * 64 + 64, :] = jnp.zeros((64, PX), BF)

    oz = offs[0, me]
    rows = iota((48, 384), 0)
    cols = iota((48, 384), 1)
    slot_n = lax.shift_right_logical(cols, 7)
    from_z = lax.shift_right_logical(cols & 127, 1)
    from_row = slot_n * 2 + (cols & 1)
    to_row = lax.shift_right_logical(rows, 3)
    low = jnp.where(sp == 0, 2, 0)
    high = jnp.where(sp == NS - 1, 3, 5)
    keep_row = (from_row == to_row) & (to_row >= low) & (to_row <= high)
    for b in range(4):
        rel = (rows & 7) + (4 * b - 1)
        hit = keep_row & (from_z == rel + oz) & (rel >= 0) & (rel < PZ)
        sels[b * 48 : b * 48 + 48, :] = jnp.where(hit, 1.0, 0.0).astype(BF)

    def wait_images(n, first):
        def body(k, c):
            image_arrival(n, group(k)).wait_recv()
            return c

        lax.fori_loop(first, NP, body, 0)

    wait_images(1, 1)

    @pl.when(above)
    def _():
        wait_images(0, 0)

    @pl.when(below)
    def _():
        wait_images(2, 0)

    rowsel = jnp.dot(sels[...], gath[...].reshape(384, PX), preferred_element_type=F32)
    lane_r = iota((192, PX), 1)
    before = jnp.where(lane_r == 0, 0.0, pltpu.roll(rowsel, 1, 1))
    after = jnp.where(lane_r == PX - 1, 0.0, pltpu.roll(rowsel, PX - 1, 1))
    for c, cells in enumerate((before, rowsel, after)):
        for b in range(4):
            cut = cells[b * 48 : b * 48 + 48].astype(BF)
            im2[b, c * 48 : c * 48 + 48, :] = cut
            im2[4 + b, (2 - c) * 48 : (2 - c) * 48 + 48, :] = cut

    def sums(parts):
        first = parts[0]
        second = parts[0] * parts[0]
        for part in parts[1:]:
            first = first + part
            second = second + part * part
        return first, second

    def to_lanes(blocks):
        cells = jnp.concatenate(blocks, axis=0)
        return jnp.sum(jnp.transpose(cells), axis=0, keepdims=True)

    own[...] = jnp.dot(w1s[:512], wide(im2, range(8)), preferred_element_type=F32)
    firsts, seconds = [], []
    for zf in range(2):
        for xf in range(2):
            one, two = sums([
                own[zf * 256 + i * 32 : zf * 256 + i * 32 + 32, xf * 512 + b * PX : xf * 512 + b * PX + PX]
                for i in range(8) for b in range(4)
            ])
            firsts.append(one)
            seconds.append(two)

    def stat_copy(buf, ssem, rsem, k):
        return pltpu.make_async_remote_copy(
            src_ref=buf.at[sp], dst_ref=buf.at[sp],
            send_sem=ssem.at[k], recv_sem=rsem.at[sp],
            device_id=(me, space(k)), device_id_type=MESH,
        )

    def stat_arrival(buf, ssem, rsem, k):
        return pltpu.make_async_remote_copy(
            src_ref=buf.at[space(k)], dst_ref=buf.at[space(k)],
            send_sem=ssem.at[k], recv_sem=rsem.at[space(k)],
            device_id=(me, space(k)), device_id_type=MESH,
        )

    def send_stats(buf, ssem, rsem):
        for k in sorted(range(1, NS), key=far):
            stat_copy(buf, ssem, rsem, k).start()

    def wait_stats(buf, ssem, rsem):
        def body(k, c):
            stat_arrival(buf, ssem, rsem, k).wait_recv()
            return c
        lax.fori_loop(1, NS, body, 0)

    def scales(buf, gain, bias):
        total = jnp.sum(buf[...], axis=0)
        cells = float(PZ * PY * PX)
        mean = total[0:1] / cells
        variance = total[1:2] / cells - mean * mean
        factor = lax.rsqrt(variance + 1e-05) * jnp.concatenate([gain[...]] * 4, axis=1)
        shift = jnp.concatenate([bias[...]] * 4, axis=1) - mean * factor
        return (
            jnp.transpose(jnp.broadcast_to(factor, (128, 128))),
            jnp.transpose(jnp.broadcast_to(shift, (128, 128))),
        )

    def leaky(u):
        return jnp.maximum(u, 0.01 * u)

    st1[sp] = jnp.concatenate([to_lanes(firsts), to_lanes(seconds)], axis=0)
    @pl.when(known < NS)
    def _():
        pl.semaphore_wait(late, NS - known)

    send_stats(st1, s_st1, r_st1)

    halo[...] = jnp.dot(w1s[512:], wide(im2, range(8)), preferred_element_type=F32)

    row16 = iota((16, 512), 0)
    col16 = iota((16, 512), 1)
    head = jnp.concatenate([hw[...].astype(F32)] * 16, axis=1)
    k16 = lax.shift_right_logical(row16 & 7, 1)
    spread = jnp.zeros((16, 512), F32)
    for k in range(3):
        spread = jnp.where(k16 == k, head[k : k + 1, :], spread)
    same = (lax.shift_right_logical(row16, 3) == (lax.shift_right_logical(col16, 6) & 1)) & (
        (row16 & 1) == (lax.shift_right_logical(col16, 5) & 1)
    )
    whs[...] = jnp.where(same, spread, 0.0).astype(BF)

    lead = iota((128, PX), 0)
    width = iota((128, PX), 1)
    row_y = (2 * sp + (lead & 1)).astype(F32)
    wmap[...] = (
        gauss(lax.shift_right_logical(lead, 3).astype(F32), PZ) * gauss(row_y, PY) * gauss(width.astype(F32), PX)
    )

    r48 = iota((48, 128), 0)
    c48 = iota((48, 128), 1)
    z48 = lax.shift_right_logical(r48 * 43, 8)
    m48 = r48 - z48 * 6
    for q in range(NP):
        hit = ((c48 & 7) == m48) & (lax.shift_right_logical(c48, 3) == z48 + 8 * q - oz)
        place[q * 48 : q * 48 + 48, :] = jnp.where(hit, 1.0, 0.0).astype(BF)

    rc = iota((48, VX), 0)
    xc = iota((48, VX), 1)
    zc = lax.shift_right_logical(rc * 43, 8)
    yc = (2 * sp + ((rc - zc * 6) & 1)).astype(F32)
    plane = jnp.zeros((48, VX), F32)
    for p in range(NP):
        rel_z = 8 * me + zc - offs[0, p]
        rel_x = xc - offs[1, p]
        inside = (rel_z >= 0) & (rel_z < PZ) & (rel_x >= 0) & (rel_x < PX)
        value = gauss(rel_z.astype(F32), PZ) * gauss(rel_x.astype(F32), PX)
        plane = plane + jnp.where(inside, value, 0.0)
    inv[...] = jnp.maximum(plane * gauss(yc, PY), 0.1)

    back = iota((PX, VX), 1) - iota((PX, VX), 0)
    for p in range(NP):
        unblend[p * PX : p * PX + PX, :] = jnp.where(back == offs[1, p], 1.0, 0.0).astype(BF)

    wait_stats(st1, s_st1, r_st1)
    factor1, shift1 = scales(st1, g1, b1)

    edge = (jnp.where(sp == 0, 0.0, 1.0), jnp.where(sp == NS - 1, 0.0, 1.0))
    lane_b = iota((CH, PX), 1)
    zero_b = jnp.zeros((CH, PX), BF)
    firsts, seconds = [], []
    for zf in range(2):
        for xf in range(2):
            f = zf * 2 + xf
            scale = factor1[f * 32 : f * 32 + 32]
            shift = shift1[f * 32 : f * 32 + 32]
            for zo in range(4):
                for row in range(4):
                    source = own if row in (1, 2) else halo
                    r = row - 1 if row in (1, 2) else row // 3
                    at = zf * 256 + zo * 64 + r * 32
                    if row in (0, 3):
                        sc, sh = scale * edge[row // 3], shift * edge[row // 3]
                    else:
                        sc, sh = scale, shift
                    zp = zo % 2
                    zi = 1 - zp if zf else zp
                    for b in range(4):
                        j = 2 * b + zo // 2
                        u = leaky(source[at : at + 32, xf * 512 + b * PX : xf * 512 + b * PX + PX] * sc + sh)
                        u = u.astype(BF)
                        prior = jnp.where(lane_b == 0, zero_b, pltpu.roll(u, 1, 1))
                        later = jnp.where(lane_b == PX - 1, zero_b, pltpu.roll(u, PX - 1, 1))
                        for c, cells in enumerate((prior, u, later)):
                            ci = 2 - c if xf else c
                            k = zi * 256 + (row * 2 + ci) * 32 if ci < 2 else 512 + (zi * 4 + row) * 32
                            act[f * 8 + j, k : k + 32, :] = cells
            tiles = range(f * 8, f * 8 + 8)
            for i, buf in enumerate((pone, ptwo)):
                weights = jnp.concatenate([w2s[2 * i + h, i * 64 : i * 64 + 192, :] for h in range(2)], axis=1)
                cells = jnp.concatenate([act[t, i * 256 : i * 256 + 256, :] for t in tiles], axis=1)
                buf[...] = jnp.dot(weights, cells, preferred_element_type=F32)
            cells = jnp.concatenate([act[t, 512:, :] for t in tiles], axis=1)
            pbuf[...] = jnp.dot(wide(w2s, (4, 5)), cells, preferred_element_type=F32)

            def slot(s, j):
                s = 3 - s if zf else s
                x = j * PX
                value = pbuf[s * 64 : s * 64 + 64, x : x + PX]
                if s < 3:
                    value = value + pone[s * 64 : s * 64 + 64, x : x + PX]
                if s > 0:
                    value = value + ptwo[s * 64 - 64 : s * 64, x : x + PX]
                return value

            parts = []
            for j in range(8):
                even = slot(1, j)
                if j > 0:
                    even = even + slot(3, j - 1)
                odd = slot(2, j)
                if j < 7:
                    odd = odd + slot(0, j + 1)
                for zp, value in enumerate((even, odd)):
                    at = f * 128 + zp * 64
                    conv[at : at + 64, j * PX : j * PX + PX] = value
                    parts.append(value[:32])
                    parts.append(value[32:])
            one, two = sums(parts)
            firsts.append(one)
            seconds.append(two)

    st2[sp] = jnp.concatenate([to_lanes(firsts), to_lanes(seconds)], axis=0)
    send_stats(st2, s_st2, r_st2)
    wait_stats(st2, s_st2, r_st2)
    factor2, shift2 = scales(st2, g2, b2)

    for f in range(4):
        scale = factor2[f * 32 : f * 32 + 32]
        shift = shift2[f * 32 : f * 32 + 32]
        for i in range(4):
            at = f * 128 + i * 32
            for j in range(8):
                u = leaky(conv[at : at + 32, j * PX : j * PX + PX] * scale + shift)
                hid[j, at : at + 32, :] = u.astype(BF)
    raw = jnp.dot(whs[...], wide(hid, range(8)), preferred_element_type=F32)
    k_of = lax.shift_right_logical(iota((16, PX), 0) & 7, 1)
    head_b = jnp.where(k_of == 0, hb[0], jnp.where(k_of == 1, hb[1], hb[2]))
    for j in range(8):
        value = (raw[:, j * PX : j * PX + PX] * 0.25 + head_b) * wmap[j * 16 : j * 16 + 16, :]
        logit[j * 16 : j * 16 + 16, :] = value.astype(BF)
    placed = jnp.dot(place[...], logit[...], preferred_element_type=F32)
    for q in range(NP):
        msend[q] = placed[q * 48 : q * 48 + 48].astype(BF)

    def out_copy(q):
        return pltpu.make_async_remote_copy(
            src_ref=msend.at[q], dst_ref=mrecv.at[me],
            send_sem=s_out.at[q], recv_sem=r_out.at[me],
            device_id=(q, sp), device_id_type=MESH,
        )

    def out_arrival(q):
        return pltpu.make_async_remote_copy(
            src_ref=msend.at[q], dst_ref=mrecv.at[q],
            send_sem=s_out.at[q], recv_sem=r_out.at[q],
            device_id=(q, sp), device_id_type=MESH,
        )

    def send_out(k, c):
        out_copy(group(k)).start()
        return c

    lax.fori_loop(1, NP, send_out, 0)
    mrecv[me] = msend[me]

    def drain_images(n, first):
        def body(k, c):
            image_copy(n, group(k)).wait_send()
            return c

        lax.fori_loop(first, NP, body, 0)

    drain_images(1, 1)

    @pl.when(below)
    def _():
        drain_images(0, 0)

    @pl.when(above)
    def _():
        drain_images(2, 0)

    def drain_stats(k, c):
        stat_copy(st1, s_st1, r_st1, k).wait_send()
        stat_copy(st2, s_st2, r_st2, k).wait_send()
        return c

    lax.fori_loop(1, NS, drain_stats, 0)

    def drain_out(k, c):
        out_copy(group(k)).wait_send()
        return c

    lax.fori_loop(1, NP, drain_out, 0)

    def wait_out(k, c):
        out_arrival(group(k)).wait_recv()
        return c

    lax.fori_loop(1, NP, wait_out, 0)


def place_kernel(mrecv, unblend, inv, out):
    got = jnp.concatenate([mrecv[p] for p in range(NP)], axis=1)
    final = jnp.dot(got, unblend[...], preferred_element_type=F32) / inv[...]
    for z in range(8):
        for k in range(3):
            out[z, k] = final[z * 6 + k * 2 : z * 6 + k * 2 + 2, :]


def local(image, offsets, w1, w2, g1, b1, g2, b2, hw, hb):
    vm = pl.BlockSpec(memory_space=pltpu.VMEM)
    hold = pl.BlockSpec(memory_space=pltpu.HBM)
    dma = pltpu.SemaphoreType.DMA
    inputs = (
        image, offsets.T, w1.transpose(0, 2, 1), w2, g1.reshape(1, CH), b1.reshape(1, CH), g2.reshape(1, CH),
        b2.reshape(1, CH), hw, hb,
    )
    blocks = pl.pallas_call(
        kernel,
        out_shape=(
            pltpu.VMEM((NP, 48, PX), BF),
            pltpu.VMEM((NP * PX, VX), BF),
            pltpu.VMEM((48, VX), F32),
        ),
        in_specs=[hold] * 10,
        out_specs=(vm, vm, vm),
        scratch_shapes=[
            pltpu.VMEM((8, 2, VX), BF),
            pltpu.SMEM((2, NP), jnp.int32),
            pltpu.VMEM((9, 3, CH), BF),
            pltpu.VMEM((9, CH, 96), BF),
            pltpu.VMEM((1, CH), F32),
            pltpu.VMEM((1, CH), F32),
            pltpu.VMEM((1, CH), F32),
            pltpu.VMEM((1, CH), F32),
            pltpu.VMEM((3, CH), BF),
            pltpu.SMEM((3,), F32),
            pltpu.VMEM((CH, CH), F32),
            pltpu.VMEM((16, VX), F32),
            pltpu.VMEM((NP, 16, PX), BF),
            pltpu.VMEM((3, NP, 16, PX), BF),
            pltpu.VMEM((1024, 144), BF),
            pltpu.VMEM((6, 256, PX), BF),
            pltpu.VMEM((16, 512), BF),
            pltpu.VMEM((192, 384), BF),
            pltpu.VMEM((8, 144, PX), BF),
            pltpu.VMEM((512, 1024), F32),
            pltpu.VMEM((512, 1024), F32),
            pltpu.VMEM((32, 768, PX), BF),
            pltpu.VMEM((192, 1024), F32),
            pltpu.VMEM((192, 1024), F32),
            pltpu.VMEM((256, 1024), F32),
            pltpu.VMEM((512, 1024), F32),
            pltpu.VMEM((8, 512, PX), BF),
            pltpu.VMEM((NS, 2, PX), F32),
            pltpu.VMEM((NS, 2, PX), F32),
            pltpu.VMEM((384, PX), BF),
            pltpu.VMEM((128, PX), F32),
            pltpu.VMEM((128, PX), BF),
            pltpu.VMEM((NP, 48, PX), BF),
            pltpu.SemaphoreType.REGULAR,
            dma((10,)), dma((3, NP)), dma((3, NP)),
            dma((NS,)), dma((NS,)), dma((NS,)), dma((NS,)),
            dma((NP,)), dma((NP,)),
        ],
        compiler_params=pltpu.CompilerParams(
            collective_id=0, has_side_effects=True, vmem_limit_bytes=40 * 1024 * 1024
        ),
    )(*[pltpu.with_memory_space_constraint(value, pltpu.HBM) for value in inputs])
    return pl.pallas_call(
        place_kernel,
        out_shape=jax.ShapeDtypeStruct((8, 3, 2, VX), F32),
        in_specs=[vm, vm, vm],
        out_specs=vm,
        compiler_params=pltpu.CompilerParams(vmem_limit_bytes=8 * 1024 * 1024),
    )(*[pltpu.with_memory_space_constraint(b, pltpu.VMEM) for b in blocks])


def solution(mesh):
    return jax.shard_map(
        local,
        mesh=mesh,
        in_specs=(P("patch", "space", None), P(), P(), P(), P(), P(), P(), P(), P(), P()),
        out_specs=P("patch", None, "space", None),
        check_vma=False,
    )
```

```python
import jax
import jax.numpy as jnp
from jax import lax
from jax.experimental import pallas as pl
from jax.experimental.pallas import tpu as pltpu
from jax.sharding import PartitionSpec as P

PX = 128
PZ = 16
CH = 32
NP = 8
NS = 32
PY = 64
VX = 256
MESH = pl.DeviceIdType.MESH
BF = jnp.bfloat16
F32 = jnp.float32
HI = lax.Precision.HIGHEST


def iota(shape, dim):
    return lax.broadcasted_iota(jnp.int32, shape, dim)


def wide(ref, blocks):
    return jnp.concatenate([ref[i] for i in blocks], axis=1)


def gauss(positions, length):
    center = (length - 1) / 2.0
    deviation = length / 8.0
    offset = positions - center
    return jnp.exp(-(offset * offset) / (2.0 * deviation * deviation))


def far(k):
    dz = (k + 1) // 4
    return -min(dz, 8 - dz) - min(k % 4, 4 - k % 4)


def kernel(
    image_in, offs_in, w1_in, w2_in, g1_in, b1_in, g2_in, b2_in, hw_in, hb_in, mrecv, unblend, inv,
    image, offs, w1, w2, g1, b1, g2, b2, hw, hb, wrow, slab, xsend, gath, w1s, w2s, whs, sels, im2, own, halo, act, pone, ptwo, pbuf, conv, hid,
    st1, st2, place, wmap, logit, msend,
    late, s_in, s_img, r_img, s_st1, r_st1, s_st2, r_st2, s_out, r_out,
):
    me = lax.axis_index("patch")
    sp = lax.axis_index("space")

    def space(k):
        return lax.rem(sp + k + NS, NS)

    def group(k):
        return lax.rem(me + k, NP)

    barrier = pltpu.get_barrier_semaphore()

    def greet(p, s):
        pl.semaphore_signal(barrier, inc=1, device_id=(p, s), device_id_type=MESH)

    above = sp > 0
    below = sp < NS - 1
    layer, rank = lax.div(sp, 4), lax.rem(sp, 4)

    def torus(dz, dy):
        return lax.rem(layer + dz + 8, 8) * 4 + lax.rem(rank + dy + 4, 4)

    order = (4, 5, 3, 2, 6, 7, 1)

    @pl.when(below)
    def _():
        for k in order + (0,):
            greet(group(k), sp + 1)

    @pl.when(above)
    def _():
        for k in order + (0,):
            greet(group(k), sp - 1)

    for k in order:
        greet(group(k), sp)
    def release(dz, dy):
        z = lax.rem(layer + dz + 8, 8)
        y = lax.rem(rank + dy + 4, 4)
        return jnp.minimum(z, 4) + jnp.minimum(y, 4 - y)

    mine = release(0, 0)
    others = sorted(
        ((dz, dy) for dz in range(-3, 5) for dy in range(-1, 3) if (dz, dy) != (0, 0)),
        key=lambda d: -abs(d[0]) - abs(d[1]),
    )

    def tell(signal, later, members):
        for dz, dy in members:
            theirs = release(dz, dy)

            @pl.when(theirs >= mine if later else theirs < mine)
            def _(dz=dz, dy=dy):
                pl.semaphore_signal(signal, inc=1, device_id=(me, torus(dz, dy)), device_id_type=MESH)

    tell(barrier, True, others)
    known = 0
    for at, count in enumerate((1, 4, 8, 12, 19, 28, 32)):
        known = jnp.where(mine == at, count, known)

    pairs = (
        (image_in, image), (offs_in, offs), (w1_in, w1), (w2_in, w2), (g1_in, g1),
        (b1_in, b1), (g2_in, g2), (b2_in, b2), (hw_in, hw), (hb_in, hb),
    )
    loads = [pltpu.make_async_copy(src, dst, s_in.at[i]) for i, (src, dst) in enumerate(pairs)]
    for load in loads:
        load.start()
    wrow[...] = jnp.zeros_like(wrow)
    for load in loads[:2]:
        load.wait()

    for z in range(8):
        slab[2 * z : 2 * z + 2, :] = image[z].astype(F32)
    diff = iota((VX, PX), 0) - iota((VX, PX), 1)
    for p in range(NP):
        pick = jnp.where(diff == offs[1, p], 1.0, 0.0).astype(BF)
        xsend[p] = jnp.dot(slab[...].astype(BF), pick, preferred_element_type=F32).astype(BF)

    near = jnp.where(above, NP, 0) + jnp.where(below, NP, 0) + NP - 1
    pl.semaphore_wait(barrier, near + known - 1)
    tell(late, False, others)

    def image_copy(n, p):
        return pltpu.make_async_remote_copy(
            src_ref=xsend.at[p], dst_ref=gath.at[n, me],
            send_sem=s_img.at[n, p], recv_sem=r_img.at[n, me],
            device_id=(p, space(1 - n)), device_id_type=MESH,
        )

    def image_arrival(n, q):
        return pltpu.make_async_remote_copy(
            src_ref=xsend.at[q], dst_ref=gath.at[n, q],
            send_sem=s_img.at[n, q], recv_sem=r_img.at[n, q],
            device_id=(q, space(1 - n)), device_id_type=MESH,
        )

    @pl.when(below)
    def _():
        for k in order + (0,):
            image_copy(0, group(k)).start()

    @pl.when(above)
    def _():
        for k in order + (0,):
            image_copy(2, group(k)).start()

    for k in order:
        image_copy(1, group(k)).start()
    gath[1, me] = xsend[me]

    @pl.when(jnp.logical_not(above))
    def _():
        gath[0] = jnp.zeros_like(gath[0])

    @pl.when(jnp.logical_not(below))
    def _():
        gath[2] = jnp.zeros_like(gath[2])

    for load in loads[2:]:
        load.wait()
    for t in range(9):
        wrow[3 * t : 3 * t + 3, :] = w1[t].astype(F32)
    lane = iota((CH, VX), 1)
    tap = iota((CH, VX), 0)
    tap_a = lax.shift_right_logical(tap * 57, 9)
    tap_r = tap - 9 * tap_a
    tap_b = lax.shift_right_logical(tap_r * 11, 5)
    tap_c = tap_r - 3 * tap_b
    for flip in range(2):
        where = tap_c * 48 + tap_b * 8 + (2 - tap_a if flip else tap_a)
        pick = jnp.where((lane == where) & (tap < 27), 1.0, 0.0).astype(BF)
        base = lax.dot_general(
            wrow[...].astype(BF), pick, (((0,), (0,)), ((), ())), preferred_element_type=F32
        )
        for part in range(2):
            for zo in range(4):
                for r in range(2):
                    row = (1 + r) if part == 0 else 3 * r
                    shift = row * 8 + zo
                    moved = base if shift == 0 else pltpu.roll(base, shift, 1)
                    at = part * 512 + flip * 256 + zo * 64 + r * 32
                    w1s[at : at + 32, :] = moved[:, :144].astype(BF)
    nothing = jnp.zeros((CH, 96), F32)
    for a in range(3):
        taps = [w2[3 * a + b].astype(F32) for b in range(3)]
        for ro in range(2):
            pieces = [nothing] + taps if ro else taps + [nothing]
            pair = jnp.concatenate([piece[:, :64] for piece in pieces], axis=1).astype(BF)
            last = jnp.concatenate([piece[:, 64:] for piece in pieces], axis=1).astype(BF)
            for zp in range(2):
                slot = zp - a + 2
                if 0 <= slot < 4:
                    at = (slot * 2 + ro) * 32
                    for i in range(2):
                        w2s[zp * 2 + i, at : at + 32, :] = pair[:, i * PX : i * PX + PX]
                    w2s[4 + zp, at : at + 32, :] = last
    for slot, zp in ((3, 0), (0, 1)):
        w2s[4 + zp, slot * 64 : slot * 64 + 64, :] = jnp.zeros((64, PX), BF)

    oz = offs[0, me]
    rows = iota((48, 384), 0)
    cols = iota((48, 384), 1)
    slot_n = lax.shift_right_logical(cols, 7)
    from_z = lax.shift_right_logical(cols & 127, 1)
    from_row = slot_n * 2 + (cols & 1)
    to_row = lax.shift_right_logical(rows, 3)
    low = jnp.where(sp == 0, 2, 0)
    high = jnp.where(sp == NS - 1, 3, 5)
    keep_row = (from_row == to_row) & (to_row >= low) & (to_row <= high)
    for b in range(4):
        rel = (rows & 7) + (4 * b - 1)
        hit = keep_row & (from_z == rel + oz) & (rel >= 0) & (rel < PZ)
        sels[b * 48 : b * 48 + 48, :] = jnp.where(hit, 1.0, 0.0).astype(BF)

    def wait_images(n, first):
        def body(k, c):
            image_arrival(n, group(k)).wait_recv()
            return c

        lax.fori_loop(first, NP, body, 0)

    wait_images(1, 1)

    @pl.when(above)
    def _():
        wait_images(0, 0)

    @pl.when(below)
    def _():
        wait_images(2, 0)

    rowsel = jnp.dot(sels[...], gath[...].reshape(384, PX), preferred_element_type=F32)
    lane_r = iota((192, PX), 1)
    before = jnp.where(lane_r == 0, 0.0, pltpu.roll(rowsel, 1, 1))
    after = jnp.where(lane_r == PX - 1, 0.0, pltpu.roll(rowsel, PX - 1, 1))
    for c, cells in enumerate((before, rowsel, after)):
        for b in range(4):
            cut = cells[b * 48 : b * 48 + 48].astype(BF)
            im2[b, c * 48 : c * 48 + 48, :] = cut
            im2[4 + b, (2 - c) * 48 : (2 - c) * 48 + 48, :] = cut

    def sums(parts):
        first = parts[0]
        second = parts[0] * parts[0]
        for part in parts[1:]:
            first = first + part
            second = second + part * part
        return first, second

    def to_lanes(blocks):
        cells = jnp.concatenate(blocks, axis=0)
        return jnp.sum(jnp.transpose(cells), axis=0, keepdims=True)

    own[...] = jnp.dot(w1s[:512], wide(im2, range(8)), preferred_element_type=F32)
    firsts, seconds = [], []
    for zf in range(2):
        for xf in range(2):
            one, two = sums([
                own[zf * 256 + i * 32 : zf * 256 + i * 32 + 32, xf * 512 + b * PX : xf * 512 + b * PX + PX]
                for i in range(8) for b in range(4)
            ])
            firsts.append(one)
            seconds.append(two)

    def stat_copy(buf, ssem, rsem, k):
        return pltpu.make_async_remote_copy(
            src_ref=buf.at[sp], dst_ref=buf.at[sp],
            send_sem=ssem.at[k], recv_sem=rsem.at[sp],
            device_id=(me, space(k)), device_id_type=MESH,
        )

    def stat_arrival(buf, ssem, rsem, k):
        return pltpu.make_async_remote_copy(
            src_ref=buf.at[space(k)], dst_ref=buf.at[space(k)],
            send_sem=ssem.at[k], recv_sem=rsem.at[space(k)],
            device_id=(me, space(k)), device_id_type=MESH,
        )

    def send_stats(buf, ssem, rsem):
        for k in sorted(range(1, NS), key=far):
            stat_copy(buf, ssem, rsem, k).start()

    def wait_stats(buf, ssem, rsem):
        def body(i, c):
            step = lax.div(i + 1, 2)
            k = jnp.where(lax.rem(i, 2) == 1, step, NS - step)
            stat_arrival(buf, ssem, rsem, k).wait_recv()
            return c

        lax.fori_loop(1, NS, body, 0)

    def scales(buf, gain, bias):
        total = jnp.sum(buf[...], axis=0)
        cells = float(PZ * PY * PX)
        mean = total[0:1] / cells
        variance = total[1:2] / cells - mean * mean
        factor = lax.rsqrt(variance + 1e-05) * jnp.concatenate([gain[...]] * 4, axis=1)
        shift = jnp.concatenate([bias[...]] * 4, axis=1) - mean * factor
        return (
            jnp.transpose(jnp.broadcast_to(factor, (128, 128))),
            jnp.transpose(jnp.broadcast_to(shift, (128, 128))),
        )

    def leaky(u):
        return jnp.maximum(u, 0.01 * u)

    st1[sp] = jnp.concatenate([to_lanes(firsts), to_lanes(seconds)], axis=0)
    @pl.when(known < NS)
    def _():
        pl.semaphore_wait(late, NS - known)

    send_stats(st1, s_st1, r_st1)

    halo[...] = jnp.dot(w1s[512:], wide(im2, range(8)), preferred_element_type=F32)

    row16 = iota((16, 512), 0)
    col16 = iota((16, 512), 1)
    head = jnp.concatenate([hw[...].astype(F32)] * 16, axis=1)
    k16 = lax.shift_right_logical(row16 & 7, 1)
    spread = jnp.zeros((16, 512), F32)
    for k in range(3):
        spread = jnp.where(k16 == k, head[k : k + 1, :], spread)
    same = (lax.shift_right_logical(row16, 3) == (lax.shift_right_logical(col16, 6) & 1)) & (
        (row16 & 1) == (lax.shift_right_logical(col16, 5) & 1)
    )
    whs[...] = jnp.where(same, spread, 0.0).astype(BF)

    lead = iota((128, PX), 0)
    width = iota((128, PX), 1)
    row_y = (2 * sp + (lead & 1)).astype(F32)
    wmap[...] = (
        gauss(lax.shift_right_logical(lead, 3).astype(F32), PZ) * gauss(row_y, PY) * gauss(width.astype(F32), PX)
    )

    r48 = iota((48, 128), 0)
    c48 = iota((48, 128), 1)
    z48 = lax.shift_right_logical(r48 * 43, 8)
    m48 = r48 - z48 * 6
    for q in range(NP):
        hit = ((c48 & 7) == m48) & (lax.shift_right_logical(c48, 3) == z48 + 8 * q - oz)
        place[q * 48 : q * 48 + 48, :] = jnp.where(hit, 1.0, 0.0).astype(BF)

    rc = iota((48, VX), 0)
    xc = iota((48, VX), 1)
    zc = lax.shift_right_logical(rc * 43, 8)
    yc = (2 * sp + ((rc - zc * 6) & 1)).astype(F32)
    plane = jnp.zeros((48, VX), F32)
    for p in range(NP):
        rel_z = 8 * me + zc - offs[0, p]
        rel_x = xc - offs[1, p]
        inside = (rel_z >= 0) & (rel_z < PZ) & (rel_x >= 0) & (rel_x < PX)
        value = gauss(rel_z.astype(F32), PZ) * gauss(rel_x.astype(F32), PX)
        plane = plane + jnp.where(inside, value, 0.0)
    inv[...] = jnp.maximum(plane * gauss(yc, PY), 0.1)

    back = iota((PX, VX), 1) - iota((PX, VX), 0)
    for p in range(NP):
        unblend[p * PX : p * PX + PX, :] = jnp.where(back == offs[1, p], 1.0, 0.0).astype(BF)

    wait_stats(st1, s_st1, r_st1)
    factor1, shift1 = scales(st1, g1, b1)

    edge = (jnp.where(sp == 0, 0.0, 1.0), jnp.where(sp == NS - 1, 0.0, 1.0))
    lane_b = iota((CH, PX), 1)
    zero_b = jnp.zeros((CH, PX), BF)
    firsts, seconds = [], []
    for zf in range(2):
        for xf in range(2):
            f = zf * 2 + xf
            scale = factor1[f * 32 : f * 32 + 32]
            shift = shift1[f * 32 : f * 32 + 32]
            for zo in range(4):
                for row in range(4):
                    source = own if row in (1, 2) else halo
                    r = row - 1 if row in (1, 2) else row // 3
                    at = zf * 256 + zo * 64 + r * 32
                    if row in (0, 3):
                        sc, sh = scale * edge[row // 3], shift * edge[row // 3]
                    else:
                        sc, sh = scale, shift
                    zp = zo % 2
                    zi = 1 - zp if zf else zp
                    for b in range(4):
                        j = 2 * b + zo // 2
                        u = leaky(source[at : at + 32, xf * 512 + b * PX : xf * 512 + b * PX + PX] * sc + sh)
                        u = u.astype(BF)
                        prior = jnp.where(lane_b == 0, zero_b, pltpu.roll(u, 1, 1))
                        later = jnp.where(lane_b == PX - 1, zero_b, pltpu.roll(u, PX - 1, 1))
                        for c, cells in enumerate((prior, u, later)):
                            ci = 2 - c if xf else c
                            k = zi * 256 + (row * 2 + ci) * 32 if ci < 2 else 512 + (zi * 4 + row) * 32
                            act[f * 8 + j, k : k + 32, :] = cells
            tiles = range(f * 8, f * 8 + 8)
            for i, buf in enumerate((pone, ptwo)):
                weights = jnp.concatenate([w2s[2 * i + h, i * 64 : i * 64 + 192, :] for h in range(2)], axis=1)
                cells = jnp.concatenate([act[t, i * 256 : i * 256 + 256, :] for t in tiles], axis=1)
                buf[...] = jnp.dot(weights, cells, preferred_element_type=F32)
            cells = jnp.concatenate([act[t, 512:, :] for t in tiles], axis=1)
            pbuf[...] = jnp.dot(wide(w2s, (4, 5)), cells, preferred_element_type=F32)

            def slot(s, j):
                s = 3 - s if zf else s
                x = j * PX
                value = pbuf[s * 64 : s * 64 + 64, x : x + PX]
                if s < 3:
                    value = value + pone[s * 64 : s * 64 + 64, x : x + PX]
                if s > 0:
                    value = value + ptwo[s * 64 - 64 : s * 64, x : x + PX]
                return value

            parts = []
            for j in range(8):
                even = slot(1, j)
                if j > 0:
                    even = even + slot(3, j - 1)
                odd = slot(2, j)
                if j < 7:
                    odd = odd + slot(0, j + 1)
                for zp, value in enumerate((even, odd)):
                    at = f * 128 + zp * 64
                    conv[at : at + 64, j * PX : j * PX + PX] = value
                    parts.append(value[:32])
                    parts.append(value[32:])
            one, two = sums(parts)
            firsts.append(one)
            seconds.append(two)

    st2[sp] = jnp.concatenate([to_lanes(firsts), to_lanes(seconds)], axis=0)
    send_stats(st2, s_st2, r_st2)
    wait_stats(st2, s_st2, r_st2)
    factor2, shift2 = scales(st2, g2, b2)

    for f in range(4):
        scale = factor2[f * 32 : f * 32 + 32]
        shift = shift2[f * 32 : f * 32 + 32]
        for i in range(4):
            at = f * 128 + i * 32
            for j in range(8):
                u = leaky(conv[at : at + 32, j * PX : j * PX + PX] * scale + shift)
                hid[j, at : at + 32, :] = u.astype(BF)
    raw = jnp.dot(whs[...], wide(hid, range(8)), preferred_element_type=F32)
    k_of = lax.shift_right_logical(iota((16, PX), 0) & 7, 1)
    head_b = jnp.where(k_of == 0, hb[0], jnp.where(k_of == 1, hb[1], hb[2]))
    for j in range(8):
        value = (raw[:, j * PX : j * PX + PX] * 0.25 + head_b) * wmap[j * 16 : j * 16 + 16, :]
        logit[j * 16 : j * 16 + 16, :] = value.astype(BF)
    placed = jnp.dot(place[...], logit[...], preferred_element_type=F32)
    for q in range(NP):
        msend[q] = placed[q * 48 : q * 48 + 48].astype(BF)

    def out_copy(q):
        return pltpu.make_async_remote_copy(
            src_ref=msend.at[q], dst_ref=mrecv.at[me],
            send_sem=s_out.at[q], recv_sem=r_out.at[me],
            device_id=(q, sp), device_id_type=MESH,
        )

    def out_arrival(q):
        return pltpu.make_async_remote_copy(
            src_ref=msend.at[q], dst_ref=mrecv.at[q],
            send_sem=s_out.at[q], recv_sem=r_out.at[q],
            device_id=(q, sp), device_id_type=MESH,
        )

    def send_out(k, c):
        out_copy(group(k)).start()
        return c

    lax.fori_loop(1, NP, send_out, 0)
    mrecv[me] = msend[me]

    def drain_images(n, first):
        def body(k, c):
            image_copy(n, group(k)).wait_send()
            return c

        lax.fori_loop(first, NP, body, 0)

    drain_images(1, 1)

    @pl.when(below)
    def _():
        drain_images(0, 0)

    @pl.when(above)
    def _():
        drain_images(2, 0)

    def drain_stats(k, c):
        stat_copy(st1, s_st1, r_st1, k).wait_send()
        stat_copy(st2, s_st2, r_st2, k).wait_send()
        return c

    lax.fori_loop(1, NS, drain_stats, 0)

    def drain_out(k, c):
        out_copy(group(k)).wait_send()
        return c

    lax.fori_loop(1, NP, drain_out, 0)

    def wait_out(k, c):
        out_arrival(group(k)).wait_recv()
        return c

    lax.fori_loop(1, NP, wait_out, 0)


def place_kernel(mrecv, unblend, inv, out):
    got = jnp.concatenate([mrecv[p] for p in range(NP)], axis=1)
    final = jnp.dot(got, unblend[...], preferred_element_type=F32) / inv[...]
    for z in range(8):
        for k in range(3):
            out[z, k] = final[z * 6 + k * 2 : z * 6 + k * 2 + 2, :]


def local(image, offsets, w1, w2, g1, b1, g2, b2, hw, hb):
    vm = pl.BlockSpec(memory_space=pltpu.VMEM)
    hold = pl.BlockSpec(memory_space=pltpu.HBM)
    dma = pltpu.SemaphoreType.DMA
    inputs = (
        image, offsets.T, w1.transpose(0, 2, 1), w2, g1.reshape(1, CH), b1.reshape(1, CH), g2.reshape(1, CH),
        b2.reshape(1, CH), hw, hb,
    )
    blocks = pl.pallas_call(
        kernel,
        out_shape=(
            pltpu.VMEM((NP, 48, PX), BF),
            pltpu.VMEM((NP * PX, VX), BF),
            pltpu.VMEM((48, VX), F32),
        ),
        in_specs=[hold] * 10,
        out_specs=(vm, vm, vm),
        scratch_shapes=[
            pltpu.VMEM((8, 2, VX), BF),
            pltpu.SMEM((2, NP), jnp.int32),
            pltpu.VMEM((9, 3, CH), BF),
            pltpu.VMEM((9, CH, 96), BF),
            pltpu.VMEM((1, CH), F32),
            pltpu.VMEM((1, CH), F32),
            pltpu.VMEM((1, CH), F32),
            pltpu.VMEM((1, CH), F32),
            pltpu.VMEM((3, CH), BF),
            pltpu.SMEM((3,), F32),
            pltpu.VMEM((CH, CH), F32),
            pltpu.VMEM((16, VX), F32),
            pltpu.VMEM((NP, 16, PX), BF),
            pltpu.VMEM((3, NP, 16, PX), BF),
            pltpu.VMEM((1024, 144), BF),
            pltpu.VMEM((6, 256, PX), BF),
            pltpu.VMEM((16, 512), BF),
            pltpu.VMEM((192, 384), BF),
            pltpu.VMEM((8, 144, PX), BF),
            pltpu.VMEM((512, 1024), F32),
            pltpu.VMEM((512, 1024), F32),
            pltpu.VMEM((32, 768, PX), BF),
            pltpu.VMEM((192, 1024), F32),
            pltpu.VMEM((192, 1024), F32),
            pltpu.VMEM((256, 1024), F32),
            pltpu.VMEM((512, 1024), F32),
            pltpu.VMEM((8, 512, PX), BF),
            pltpu.VMEM((NS, 2, PX), F32),
            pltpu.VMEM((NS, 2, PX), F32),
            pltpu.VMEM((384, PX), BF),
            pltpu.VMEM((128, PX), F32),
            pltpu.VMEM((128, PX), BF),
            pltpu.VMEM((NP, 48, PX), BF),
            pltpu.SemaphoreType.REGULAR,
            dma((10,)), dma((3, NP)), dma((3, NP)),
            dma((NS,)), dma((NS,)), dma((NS,)), dma((NS,)),
            dma((NP,)), dma((NP,)),
        ],
        compiler_params=pltpu.CompilerParams(
            collective_id=0, has_side_effects=True, vmem_limit_bytes=40 * 1024 * 1024
        ),
    )(*[pltpu.with_memory_space_constraint(value, pltpu.HBM) for value in inputs])
    return pl.pallas_call(
        place_kernel,
        out_shape=jax.ShapeDtypeStruct((8, 3, 2, VX), F32),
        in_specs=[vm, vm, vm],
        out_specs=vm,
        compiler_params=pltpu.CompilerParams(vmem_limit_bytes=8 * 1024 * 1024),
    )(*[pltpu.with_memory_space_constraint(b, pltpu.VMEM) for b in blocks])


def solution(mesh):
    return jax.shard_map(
        local,
        mesh=mesh,
        in_specs=(P("patch", "space", None), P(), P(), P(), P(), P(), P(), P(), P(), P()),
        out_specs=P("patch", None, "space", None),
        check_vma=False,
    )
```
